512 devices in a mesh: lat: 8 (over y), lon: 32 (over x, z_hi, core), lev: 2 (over z_lo).
Axes of the slice: x: 4, y: 8, z: 8 (z_hi: 4, z_lo: 2; z = z_hi * 2 + z_lo), core: 2. Of those that a mesh axis runs over, the one named last changes fastest.
Arguments:
- tokens: bfloat16 [4, 48, 384, 192], P('lev', 'lat', 'lon'), may hold values from -6 to 6
- norm1_gain: float32 [192], replicated, may hold values from 0.8 to 10
- qkv_weight: bfloat16 [192, 576], replicated, may hold values from -0.4375 to 0.4375
- proj_weight: bfloat16 [192, 192], replicated, may hold values from -0.4375 to 0.4375
- earth_bias: bfloat16 [2, 8, 6, 3312], P(None, 'lat'), may hold values from -4 to 4
- norm2_gain: float32 [192], replicated, may hold values from 0.5 to 1.5
- fc1_weight: bfloat16 [192, 768], replicated, may hold values from -0.4375 to 0.4375
- fc2_weight: bfloat16 [768, 192], replicated, may hold values from -0.21875 to 0.21875
Outputs:
- blended: bfloat16 [4, 48, 384, 192], P('lev', 'lat', 'lon')
The draws below stay inside these ranges and needn't reach their ends.
All inputs are finite; a program needn't handle non-finite values.
Results may differ from the reference program's by a relative error of at most 0.008.
The reference program's roundings to bfloat16 on the way count: a program that leaves them out, or rounds other values in their place, can miss the bound.
Values may be sent and summed in bfloat16 or wider, within the bound.
No kernel may reach another device: no remote copies, remote signals or barrier semaphores. Data moves between devices by JAX's collectives and lax.ppermute only.
A program may use at most 64 MiB of HBM per device.

```python
import jax
import jax.numpy as jnp
from jax import lax

D = 192
HEADS = 6
FF = 768
WLV = 2
WLA = 6
WLO = 12
POS = 3312
NLEV = 4
NLAT = 48
NLON = 384
NWLEV = 2
NWLAT = 8


def draw_norm1_gain(key, part):
    second_key = jax.random.fold_in(jax.random.fold_in(key, 11), 1)
    return jax.random.uniform(second_key, (D,), jnp.float32, 0.8, 1.25)


def steps_of(own_key, dims, cuts, smallest, high):
    level = 1.0
    for axis_at, parts in cuts:
        draws = jax.random.uniform(jax.random.fold_in(jax.random.fold_in(own_key, 6), axis_at), (parts,), jnp.float32, smallest / len(cuts), high / len(cuts))
        level = level * jnp.repeat(jnp.exp(draws), dims[axis_at] // parts).reshape((-1,) + (1,) * (len(dims) - 1 - axis_at))
    return level


def centred(key, shape, width, limit, shards=(), held_as=jnp.bfloat16):
    loudness = steps_of(key, shape, shards, -0.22, 0.18) if shards else 1.0
    entries = jax.random.normal(key, shape, jnp.float32) * width * loudness
    return jnp.minimum(jnp.maximum(entries, -limit), limit).astype(held_as)


def setup_inputs(seed: int = 0) -> dict:
    splits = jax.random.split(jax.random.key(seed), 9)
    return {
        "tokens": centred(splits[0], (NLEV, NLAT, NLON, D), 1.0, 6.0, ((0, 2), (1, 8), (2, 32))),
        "norm1_gain": draw_norm1_gain(jax.random.fold_in(splits[8], 71), 0),
        "qkv_weight": centred(splits[2], (D, 3 * D), D ** -0.5, 0.4375),
        "proj_weight": centred(splits[3], (D, D), D ** -0.5, 0.4375),
        "earth_bias": centred(splits[4], (NWLEV, NWLAT, HEADS, POS), 1.0, 4.0, ((1, 8),)),
        "norm2_gain": jnp.clip(1.0 + 0.1 * jax.random.normal(splits[5], (D,), jnp.float32), 0.5, 1.5),
        "fc1_weight": centred(splits[6], (D, FF), D ** -0.5, 0.4375),
        "fc2_weight": centred(splits[7], (FF, D), FF ** -0.5, 0.21875),
    }


norm_eps = 1e-05

def layer_norm(values, scale_gain):
    average = lax.optimization_barrier(jnp.mean(values, axis=-1, keepdims=True))
    centered = values - average
    variance = lax.optimization_barrier(jnp.mean(centered * centered, axis=-1, keepdims=True))
    return centered * lax.rsqrt(variance + norm_eps) * scale_gain

def window_coords():
    places = jnp.arange(WLV * WLA * WLO, dtype=jnp.int32)
    return (places // (WLA * WLO), places // WLO % WLA, places % WLO)

def bias_index():
    lev_place, lat_place, lon_place = window_coords()
    paired = (lev_place[:, None] * WLV + lev_place[None, :]) * WLA + lat_place[:, None]
    paired = paired * WLA + lat_place[None, :]
    return (paired * (2 * WLO - 1) + lon_place[:, None] - lon_place[None, :] + WLO - 1).astype(jnp.int32)

def region_of(places, extent, window):
    return jnp.where(places < extent - window, 0, jnp.where(places < extent - window // 2, 1, 2)).astype(jnp.int32)

def attend_windows(windows, qkv_weight, bias_terms, allowed):
    window_count, window_size, feature_width = windows.shape
    head_dim = feature_width // HEADS
    projected = jnp.dot(windows.reshape(window_count * window_size, feature_width), qkv_weight, preferred_element_type=jnp.float32)
    projected = lax.optimization_barrier(projected.astype(jnp.bfloat16))
    projected = projected.reshape(window_count, window_size, 3, HEADS, head_dim).astype(jnp.float32)
    queries = projected[:, :, 0]
    key_rows = projected[:, :, 1]
    value_rows = projected[:, :, 2]
    scores = jnp.einsum('wqhd,wkhd->whqk', queries, key_rows) * head_dim ** (-0.5) + bias_terms
    scores = jnp.where(allowed[:, None], scores, -1e+30)
    row_max = lax.optimization_barrier(jnp.max(scores, axis=-1, keepdims=True))
    weights = jnp.exp(scores - row_max)
    probs = weights / lax.optimization_barrier(jnp.sum(weights, axis=-1, keepdims=True))
    probs = lax.optimization_barrier(probs.astype(jnp.bfloat16))
    context = jnp.einsum('whqk,wkhd->wqhd', probs.astype(jnp.float32), value_rows)
    return context.astype(jnp.bfloat16).reshape(window_count, window_size, feature_width)

def reference(tokens, norm1_gain, qkv_weight, proj_weight, earth_bias, norm2_gain, fc1_weight, fc2_weight):
    half_lev, half_lat, half_lon = (WLV // 2, WLA // 2, WLO // 2)
    normed = layer_norm(tokens.astype(jnp.float32), norm1_gain).astype(jnp.bfloat16)
    rolled = jnp.roll(normed, (-half_lev, -half_lat, -half_lon), axis=(0, 1, 2))
    table_index = bias_index()
    lev_place, lat_place, lon_place = window_coords()
    lon_windows = NLON // WLO
    window_size = WLV * WLA * WLO

    def one_band(flat_index):
        lev_window = flat_index // NWLAT
        lat_window = flat_index % NWLAT
        zero = jnp.zeros((), jnp.int32)
        banded = lax.dynamic_slice(rolled, (lev_window * WLV, lat_window * WLA, zero, zero), (WLV, WLA, NLON, D))
        windows = banded.reshape(WLV, WLA, lon_windows, WLO, D).transpose(2, 0, 1, 3, 4)
        windows = windows.reshape(lon_windows, window_size, D)
        tables = earth_bias[lev_window, lat_window]
        bias_terms = jnp.take(tables, table_index, axis=1).astype(jnp.float32)
        lev_region = region_of(lev_window * WLV + lev_place, NLEV, WLV)
        lat_region = region_of(lat_window * WLA + lat_place, NLAT, WLA)
        allowed = (lev_region[:, None] == lev_region[None, :]) & (lat_region[:, None] == lat_region[None, :])
        context = attend_windows(windows, qkv_weight, bias_terms[None], allowed[None])
        context = context.reshape(lon_windows, WLV, WLA, WLO, D).transpose(1, 2, 0, 3, 4)
        return context.reshape(WLV, WLA, NLON, D)
    bands = lax.map(one_band, jnp.arange(NWLEV * NWLAT, dtype=jnp.int32))
    context = bands.reshape(NWLEV, NWLAT, WLV, WLA, NLON, D).transpose(0, 2, 1, 3, 4, 5)
    context = context.reshape(NLEV, NLAT, NLON, D)
    context = jnp.roll(context, (half_lev, half_lat, half_lon), axis=(0, 1, 2))

    def one_level(paired_level):
        own_level, mixed_level = paired_level
        first = own_level.reshape(-1, D).astype(jnp.float32) + jnp.dot(mixed_level.reshape(-1, D), proj_weight, preferred_element_type=jnp.float32)
        normed_two = layer_norm(first, norm2_gain).astype(jnp.bfloat16)
        hidden = jax.nn.gelu(jnp.dot(normed_two, fc1_weight, preferred_element_type=jnp.float32), approximate=False).astype(jnp.bfloat16)
        result = first + jnp.dot(hidden, fc2_weight, preferred_element_type=jnp.float32)
        return result.astype(jnp.bfloat16).reshape(own_level.shape)
    return lax.map(one_level, (tokens, context))
```

```python
import numpy as np
import jax
import jax.numpy as jnp
from jax import lax
from jax.experimental import pallas as pl
from jax.experimental.pallas import tpu as pltpu
from jax.sharding import PartitionSpec as P

D = 192
HEADS = 6
HEAD_DIM = 32
WLA = 6
WLO = 12
HLA = 3
HLO = 6
SPAN = 2 * WLO - 1
ROWS = 288
HALF = 144
QROWS = 288
GROUP = 24
FAR = -1e30

norm_eps = 1e-05


def constants():
    column = np.arange(24)
    place = np.arange(WLA)
    spread = np.zeros((WLO, WLA * SPAN, HALF), np.float32)
    for o in range(WLO):
        for k in column:
            d = o - k + 17
            if (o < HLO) == (k < WLO):
                spread[o, place * SPAN + d, place * 24 + k] = 1
    pick = np.zeros((2, QROWS, HALF), np.float32)
    back = np.zeros((72, 2 * QROWS), np.float32)
    owned = np.zeros((QROWS, D), np.float32)
    for o in range(WLO):
        for h in range(HEADS):
            for a in range(4):
                row = o * GROUP + h * 4 + a
                owned[row, h * HEAD_DIM : (h + 1) * HEAD_DIM] = 1
                if a < HLA:
                    pick[0, row, (HLA + a) * 24 + HLO + o] = 1
                    pick[1, row, a * 24 + HLO + o] = 1
                    back[a * WLO + o, row] = 1
                    back[(HLA + a) * WLO + o, QROWS + row] = 1
    side = (np.arange(HALF) % 24 >= WLO).astype(np.float32).reshape(1, HALF)
    return spread, pick, back, owned, side


def normalized(values, gain):
    average = jnp.mean(values, axis=-1, keepdims=True)
    centered = values - average
    variance = jnp.mean(centered * centered, axis=-1, keepdims=True)
    return centered * lax.rsqrt(variance + norm_eps) * gain


def dot(a, b):
    return jnp.dot(a, b, preferred_element_type=jnp.float32)


def dot_t(a, b):
    return lax.dot_general(a, b, (((1,), (1,)), ((), ())), preferred_element_type=jnp.float32)


def block_kernel(
    where_ref,
    wide_ref,
    other_ref,
    own_ref,
    table_ref,
    gain1_ref,
    qkv_ref,
    proj_ref,
    gain2_ref,
    fc1_ref,
    fc2_ref,
    spread_ref,
    pick_ref,
    back_ref,
    owned_ref,
    side_ref,
    out_ref,
):
    lev = where_ref[0]
    lat = where_ref[1]
    lat_last = where_ref[2]
    gain1 = gain1_ref[...]
    w_q = qkv_ref[:, :D]
    w_k = qkv_ref[:, D : 2 * D]
    w_v = qkv_ref[:, 2 * D :]

    def normed(rows):
        return normalized(rows.astype(jnp.float32), gain1).astype(jnp.bfloat16)

    n_alone = normed(wide_ref[lev])
    n_pair = normed(wide_ref[1 - lev])
    n_other = normed(other_ref[...])

    table = table_ref[...]
    spreads = [dot(table, spread_ref[o]) for o in range(WLO)]
    row_half = lax.broadcasted_iota(jnp.int32, (QROWS, HALF), 0) >= QROWS // 2
    lane = lax.broadcasted_iota(jnp.int32, (QROWS, HALF), 1)
    side = jnp.broadcast_to(side_ref[...], (QROWS, HALF)) > 0.5
    same_side = row_half == side

    def bias_of(lat_window, entry, allowed):
        at = (lat_window * 3 + entry) * GROUP
        terms = jnp.concatenate([s[at : at + GROUP] for s in spreads], axis=0)
        return jnp.where(allowed, terms, FAR)

    owned = owned_ref[...]
    scale = HEAD_DIM**-0.5

    def level(n_self, n_extra, entries):
        queries = dot(n_self, w_q).astype(jnp.bfloat16)
        sources = [n_self] if n_extra is None else [n_self, n_extra]
        keys = [dot(n, w_k).astype(jnp.bfloat16) for n in sources]
        values = [dot(n, w_v).astype(jnp.bfloat16) for n in sources]
        parts = []
        for lat_window in range(2):
            rows = slice(lat_window * HALF, (lat_window + 1) * HALF)
            if lat_window == 0:
                near = (lane >= 72) | (lat > 0)
            else:
                near = (lane < 72) | (lat < lat_last)
            allowed = same_side & near
            spread_q = dot(pick_ref[lat_window], queries[rows]).astype(jnp.bfloat16) * owned
            scores = [
                dot_t(spread_q, k[rows]) * scale + bias_of(lat_window, e, allowed)
                for k, e in zip(keys, entries)
            ]
            top = jnp.max(scores[0], axis=-1, keepdims=True)
            for s in scores[1:]:
                top = jnp.maximum(top, jnp.max(s, axis=-1, keepdims=True))
            weights = [jnp.exp(s - top) for s in scores]
            total = jnp.sum(weights[0], axis=-1, keepdims=True)
            for w in weights[1:]:
                total = total + jnp.sum(w, axis=-1, keepdims=True)
            inverse = 1.0 / total
            context = 0.0
            for w, v in zip(weights, values):
                context = context + dot((w * inverse).astype(jnp.bfloat16), v[rows])
            parts.append(context.astype(jnp.bfloat16) * owned)
        return dot(back_ref[...], jnp.concatenate(parts, axis=0)).astype(jnp.bfloat16)

    context = jnp.concatenate(
        [level(n_alone, None, (0,)), level(n_pair, n_other, (1, 2))], axis=0
    )
    own = jnp.concatenate([own_ref[lev], own_ref[1 - lev]], axis=0).astype(jnp.float32)
    first = own + dot(context, proj_ref[...])
    normed_two = normalized(first, gain2_ref[...]).astype(jnp.bfloat16)
    mixed = dot(normed_two, fc1_ref[...])
    hidden = (mixed * (1.0 + lax.erf(mixed * (0.5**0.5))) * 0.5).astype(jnp.bfloat16)
    result = (first + dot(hidden, fc2_ref[...])).astype(jnp.bfloat16)
    out_ref[lev] = result[:72]
    out_ref[1 - lev] = result[72:]


def swapped(block, axis, crossed):
    size = lax.axis_size(axis)
    route = []
    for i in range(size):
        mate = i ^ 1 if not crossed else (i + 1 if i % 2 else i - 1) % size
        route.append((mate, i))
    return lax.ppermute(block, axis, route)


def per_device(
    tokens, norm1_gain, qkv_weight, proj_weight, earth_bias, norm2_gain, fc1_weight, fc2_weight
):
    lev = lax.axis_index("lev")
    lat = lax.axis_index("lat")
    lat_size = lax.axis_size("lat")
    lon_even = lax.axis_index("lon") % 2 == 0
    lat_even = lat % 2 == 0

    to_near = jnp.where(lon_even, tokens[:, :, HLO:], tokens[:, :, :HLO])
    to_far = jnp.where(lon_even, tokens[:, :, :HLO], tokens[:, :, HLO:])
    from_far = swapped(to_far, "lon", True)
    from_near = swapped(to_near, "lon", False)
    left = jnp.where(lon_even, from_far, from_near)
    right = jnp.where(lon_even, from_near, from_far)
    wide = jnp.concatenate([left, tokens, right], axis=2)

    tables = earth_bias[:, 0].reshape(2, HEADS, 4, WLA, WLA * SPAN)
    chosen = jnp.stack(
        [
            lax.dynamic_index_in_dim(tables[1], 3 - 3 * lev, 1, False),
            lax.dynamic_index_in_dim(tables[0], 3 * lev, 1, False),
            lax.dynamic_index_in_dim(tables[0], lev + 1, 1, False),
        ]
    )
    chosen = jnp.pad(chosen, ((0, 0), (0, 0), (0, 0), (0, D - WLA * SPAN)))
    lower = chosen[:, :, :HLA].reshape(3 * HEADS * HLA, D)
    upper = chosen[:, :, HLA:].reshape(3 * HEADS * HLA, D)

    head = wide[:, :HLA].reshape(-1, D)
    tail = wide[:, HLA:].reshape(-1, D)
    to_next = jnp.concatenate([tail, upper], axis=0)
    to_prev = jnp.pad(head, ((0, upper.shape[0]), (0, 0)))
    lat_far = swapped(jnp.where(lat_even, to_prev, to_next), "lat", True)
    lat_near = swapped(jnp.where(lat_even, to_next, to_prev), "lat", False)
    before = jnp.where(lat_even, lat_far, lat_near)
    after = jnp.where(lat_even, lat_near, lat_far)
    cells = head.shape[0]
    edges = (2, HLA * 24, D)
    extended = jnp.concatenate(
        [
            before[:cells].reshape(edges),
            wide.reshape(2, -1, D),
            after[:cells].reshape(edges),
        ],
        axis=1,
    )
    other = swapped(lax.dynamic_index_in_dim(extended, 1 - lev, 0, False), "lev", False)

    table = jnp.stack([before[cells:], lower])[:, :, : WLA * SPAN]
    table = table.reshape(2 * 3 * HEADS, HLA, WLA * SPAN)
    table = jnp.pad(table, ((0, 0), (0, 1), (0, 0))).reshape(2 * 3 * GROUP, WLA * SPAN)

    spread, pick, back, owned, side = constants()
    half = lambda a: jnp.asarray(a, jnp.bfloat16)
    whole = pl.BlockSpec(memory_space=pltpu.VMEM)
    result = pl.pallas_call(
        block_kernel,
        out_shape=jax.ShapeDtypeStruct((2, 72, D), jnp.bfloat16),
        in_specs=[pl.BlockSpec(memory_space=pltpu.SMEM)] + [whole] * 15,
        out_specs=whole,
        name="block",
    )(
        jnp.stack([lev, lat, jnp.int32(lat_size - 1)]).astype(jnp.int32),
        extended,
        other,
        tokens.reshape(2, 72, D),
        table,
        norm1_gain.reshape(1, D),
        qkv_weight,
        proj_weight,
        norm2_gain.reshape(1, D),
        fc1_weight,
        fc2_weight,
        half(spread),
        half(pick),
        half(back),
        half(owned),
        jnp.asarray(side),
    )
    return result.reshape(tokens.shape)


def solution(mesh):
    placed = (
        P("lev", "lat", "lon", None),
        P(),
        P(),
        P(),
        P(None, "lat", None, None),
        P(),
        P(),
        P(),
    )
    return jax.shard_map(
        per_device,
        mesh=mesh,
        in_specs=placed,
        out_specs=P("lev", "lat", "lon", None),
        check_vma=False,
    )
```

```python
import numpy as np
import jax
import jax.numpy as jnp
from jax import lax
from jax.experimental import pallas as pl
from jax.experimental.pallas import tpu as pltpu
from jax.sharding import PartitionSpec as P

D = 192
HEADS = 6
HEAD_DIM = 32
WLA = 6
WLO = 12
HLA = 3
HLO = 6
SPAN = 2 * WLO - 1
ROWS = 288
HALF = 144
QROWS = 288
GROUP = 24
FAR = -1e30
LANES = 256
VMEM_LIMIT = 16 * 1024 * 1024

norm_eps = 1e-05


def constants():
    column = np.arange(24)
    place = np.arange(WLA)
    spread = np.zeros((WLO, D, HALF), np.float32)
    for o in range(WLO):
        for k in column:
            d = o - k + 17
            if (o < HLO) == (k < WLO):
                spread[o, place * SPAN + d, place * 24 + k] = 1
    pick = np.zeros((2, QROWS, HALF), np.float32)
    back = np.zeros((72, 2 * QROWS), np.float32)
    owned = np.zeros((QROWS, D), np.float32)
    mine = np.zeros((72, ROWS), np.float32)
    for o in range(WLO):
        for a in range(WLA):
            mine[a * WLO + o, (HLA + a) * 24 + HLO + o] = 1
        for h in range(HEADS):
            for a in range(4):
                row = o * GROUP + h * 4 + a
                owned[row, h * HEAD_DIM : (h + 1) * HEAD_DIM] = 1
                if a < HLA:
                    pick[0, row, (HLA + a) * 24 + HLO + o] = 1
                    pick[1, row, a * 24 + HLO + o] = 1
                    back[a * WLO + o, row] = 1
                    back[(HLA + a) * WLO + o, QROWS + row] = 1
    gaps = np.zeros((3 * GROUP, 3 * HEADS * HLA), np.float32)
    for e in range(3 * HEADS):
        for a in range(HLA):
            gaps[e * 4 + a, e * HLA + a] = 1
    woven = np.zeros((2, 144, 72), np.float32)
    cell = np.arange(72)
    for at in range(2):
        woven[at, 2 * cell + at, cell] = 1
    side = (np.arange(HALF) % 24 >= WLO).astype(np.float32).reshape(1, HALF)
    return spread, pick, back, owned, mine, gaps, woven, side


def normalized(values, gain):
    average = jnp.mean(values, axis=-1, keepdims=True)
    centered = values - average
    variance = jnp.mean(centered * centered, axis=-1, keepdims=True)
    return centered * lax.rsqrt(variance + norm_eps) * gain


def dot(a, b):
    return jnp.dot(a, b, preferred_element_type=jnp.float32)


def dot_t(a, b):
    return lax.dot_general(a, b, (((1,), (1,)), ((), ())), preferred_element_type=jnp.float32)


def halved(x):
    return x.astype(jnp.bfloat16)


def softmax_context(scores, values, owned):
    top = jnp.max(scores[0], axis=-1, keepdims=True)
    for s in scores[1:]:
        top = jnp.maximum(top, jnp.max(s, axis=-1, keepdims=True))
    weights = [jnp.exp(s - top) for s in scores]
    total = jnp.sum(weights[0], axis=-1, keepdims=True)
    for w in weights[1:]:
        total = total + jnp.sum(w, axis=-1, keepdims=True)
    inverse = 1.0 / total
    context = 0.0
    for w, v in zip(weights, values):
        context = context + dot(halved(w * inverse), v)
    return halved(context) * owned


def finish(own, parts, back, proj, gain, fc1, fc2_t):
    context = halved(dot(back, jnp.concatenate(parts, axis=0)))
    first = own + dot(context, proj)
    mixed = dot(halved(normalized(first, gain)), fc1)
    hidden = halved(mixed * (1.0 + lax.erf(mixed * (0.5**0.5))) * 0.5)
    return halved(first + dot_t(hidden, fc2_t))


def early_kernel(
    wide_ref,
    before_ref,
    lower_ref,
    gain1_ref,
    qkv_ref,
    proj_ref,
    gain2_ref,
    fc1_ref,
    fc2_ref,
    spread_ref,
    pick_ref,
    back_ref,
    owned_ref,
    mine_ref,
    gaps_ref,
    side_ref,
    alone_ref,
    own_ref,
    asked_ref,
    value_ref,
    score_ref,
    bias_ref,
):
    lev = lax.axis_index("lev")
    lat = lax.axis_index("lat")
    lat_last = lax.axis_size("lat") - 1
    gain1 = gain1_ref[...]
    w_q = qkv_ref[:, :D]
    w_k = qkv_ref[:, D : 2 * D]
    w_v = qkv_ref[:, 2 * D :]
    owned = owned_ref[...]

    gaps = gaps_ref[...]
    cells = 2 * HLA * 24
    table = halved(
        jnp.concatenate(
            [
                dot(gaps, before_ref[cells : cells + 3 * HEADS * HLA, :D]),
                dot(gaps, lower_ref[:, :D]),
            ],
            axis=0,
        )
    )
    spreads = [dot(table, spread_ref[o]) for o in range(WLO)]
    row_half = lax.broadcasted_iota(jnp.int32, (QROWS, HALF), 0) >= QROWS // 2
    lane = lax.broadcasted_iota(jnp.int32, (QROWS, HALF), 1)
    side = jnp.broadcast_to(side_ref[...], (QROWS, HALF)) > 0.5
    same_side = row_half == side
    allowed = [
        same_side & ((lane >= 72) | (lat > 0)),
        same_side & ((lane < 72) | (lat < lat_last)),
    ]

    def bias_of(lat_window, entry):
        at = (lat_window * 3 + entry) * GROUP
        terms = jnp.concatenate([s[at : at + GROUP] for s in spreads], axis=0)
        return jnp.where(allowed[lat_window], terms, FAR)

    def asked_of(cells):
        n = halved(normalized(cells.astype(jnp.float32), gain1))
        queries = halved(dot(n, w_q))
        keys = halved(dot(n, w_k))
        values = halved(dot(n, w_v))
        out = []
        for lat_window in range(2):
            rows = slice(lat_window * HALF, (lat_window + 1) * HALF)
            asked = halved(dot(pick_ref[lat_window], queries[rows])) * owned
            out.append((asked, dot_t(asked, keys[rows]) * HEAD_DIM**-0.5, values[rows]))
        return out

    pair_cells = wide_ref[1 - lev]
    for lat_window, (asked, scores, values) in enumerate(asked_of(pair_cells)):
        asked_ref[lat_window] = asked
        value_ref[lat_window] = values
        score_ref[lat_window] = scores + bias_of(lat_window, 1)
        bias_ref[lat_window] = bias_of(lat_window, 2)
    own_ref[...] = dot(mine_ref[...], pair_cells)

    alone_cells = wide_ref[lev]
    parts = []
    for lat_window, (asked, scores, values) in enumerate(asked_of(alone_cells)):
        parts.append(softmax_context([scores + bias_of(lat_window, 0)], [values], owned))
    alone_ref[...] = finish(
        dot(mine_ref[...], alone_cells),
        parts,
        back_ref[...],
        proj_ref[...],
        gain2_ref[...],
        fc1_ref[...],
        fc2_ref[...],
    )


def late_kernel(
    other_ref,
    alone_ref,
    own_ref,
    asked_ref,
    value_ref,
    score_ref,
    bias_ref,
    gain1_ref,
    qkv_ref,
    proj_ref,
    gain2_ref,
    fc1_ref,
    fc2_ref,
    back_ref,
    owned_ref,
    woven_ref,
    out_ref,
):
    lev = lax.axis_index("lev")
    owned = owned_ref[...]
    n = halved(normalized(other_ref[...].astype(jnp.float32), gain1_ref[...]))
    keys = halved(dot(n, qkv_ref[:, D : 2 * D]))
    values = halved(dot(n, qkv_ref[:, 2 * D :]))
    parts = []
    for lat_window in range(2):
        rows = slice(lat_window * HALF, (lat_window + 1) * HALF)
        scores = dot_t(asked_ref[lat_window], keys[rows]) * HEAD_DIM**-0.5 + bias_ref[lat_window]
        parts.append(
            softmax_context(
                [score_ref[lat_window], scores], [value_ref[lat_window], values[rows]], owned
            )
        )
    pair = finish(
        own_ref[...],
        parts,
        back_ref[...],
        proj_ref[...],
        gain2_ref[...],
        fc1_ref[...],
        fc2_ref[...],
    )
    alone = alone_ref[...]
    lower = jnp.where(lev == 0, alone, pair)
    upper = jnp.where(lev == 0, pair, alone)
    result = halved(dot(woven_ref[0], lower) + dot(woven_ref[1], upper))
    out_ref[...] = result.reshape(72, 2, D)


def pairs_of(size, crossed):
    shift = 1 if crossed else 0
    return [[(2 * i + shift) % size, (2 * i + 1 + shift) % size] for i in range(size // 2)]


def swapped(block, axis, crossed):
    route = []
    for a, b in pairs_of(lax.axis_size(axis), crossed):
        route += [(a, b), (b, a)]
    return lax.ppermute(block, axis, route)


def per_device(
    tokens, norm1_gain, qkv_weight, proj_weight, earth_bias, norm2_gain, fc1_weight, fc2_weight
):
    lev = lax.axis_index("lev")
    lat = lax.axis_index("lat")
    lon_size = lax.axis_size("lon")
    lat_size = lax.axis_size("lat")
    lon_even = lax.axis_index("lon") % 2 == 0
    lat_even = lat % 2 == 0

    far = swapped(jnp.where(lon_even, tokens[:, :, :HLO], tokens[:, :, HLO:]), "lon", True)
    joint = lax.all_gather(
        tokens, "lon", axis_index_groups=pairs_of(lon_size, False), axis=2, tiled=True
    )
    wide = jnp.where(
        lon_even,
        jnp.concatenate([far, joint[:, :, : WLO + HLO]], axis=2),
        jnp.concatenate([joint[:, :, HLO:], far], axis=2),
    )

    tables = earth_bias[:, 0].reshape(2, HEADS, 4, WLA, WLA * SPAN)
    chosen = jnp.stack(
        [
            lax.dynamic_index_in_dim(tables[1], 3 - 3 * lev, 1, False),
            lax.dynamic_index_in_dim(tables[0], 3 * lev, 1, False),
            lax.dynamic_index_in_dim(tables[0], lev + 1, 1, False),
        ]
    )
    chosen = jnp.pad(chosen, ((0, 0), (0, 0), (0, 0), (0, LANES - WLA * SPAN)))
    lower = chosen[:, :, :HLA].reshape(3 * HEADS * HLA, LANES)
    upper = chosen[:, :, HLA:].reshape(3 * HEADS * HLA, LANES)

    head = wide[:, :HLA].reshape(-1, D)
    tail = wide[:, HLA:].reshape(-1, D)
    cells = head.shape[0]
    to_next = jnp.concatenate([jnp.pad(tail, ((0, 0), (0, LANES - D))), upper], axis=0)
    to_prev = jnp.pad(head, ((0, upper.shape[0]), (0, LANES - D)))
    lat_far = swapped(jnp.where(lat_even, to_prev, to_next), "lat", True)
    lat_both = lax.all_gather(
        jnp.where(lat_even, to_next, to_prev), "lat", axis_index_groups=pairs_of(lat_size, False)
    )
    lat_near = jnp.where(lat_even, lat_both[1], lat_both[0])
    before = jnp.where(lat_even, lat_far, lat_near)
    after = jnp.where(lat_even, lat_near, lat_far)
    edges = (2, HLA * 24, D)
    extended = jnp.concatenate(
        [
            before[:cells, :D].reshape(edges),
            wide.reshape(2, -1, D),
            after[:cells, :D].reshape(edges),
        ],
        axis=1,
    )
    other = swapped(lax.dynamic_index_in_dim(extended, 1 - lev, 0, False), "lev", False)

    spread, pick, back, owned, mine, gaps, woven = [
        jnp.asarray(a, jnp.bfloat16) for a in constants()[:-1]
    ]
    side = jnp.asarray(constants()[-1])
    whole = pl.BlockSpec(memory_space=pltpu.VMEM)
    held = lambda x: pltpu.with_memory_space_constraint(x, pltpu.VMEM)
    shared = [
        held(a)
        for a in (
            norm1_gain.reshape(1, D),
            qkv_weight,
            proj_weight,
            norm2_gain.reshape(1, D),
            fc1_weight,
            fc2_weight.T,
        )
    ]
    back = held(back)
    owned = held(owned)
    passed = [
        pltpu.VMEM((72, D), jnp.bfloat16),
        pltpu.VMEM((72, D), jnp.float32),
        pltpu.VMEM((2, QROWS, D), jnp.bfloat16),
        pltpu.VMEM((2, HALF, D), jnp.bfloat16),
        pltpu.VMEM((2, QROWS, HALF), jnp.float32),
        pltpu.VMEM((2, QROWS, HALF), jnp.float32),
    ]
    early = pl.pallas_call(
        early_kernel,
        out_shape=passed,
        in_specs=[whole] * 16,
        out_specs=[whole] * 6,
        cost_estimate=pl.CostEstimate(flops=4_000_000_000, transcendentals=0, bytes_accessed=0),
        compiler_params=pltpu.CompilerParams(vmem_limit_bytes=VMEM_LIMIT),
        name="early",
    )(
        held(extended),
        held(before),
        held(lower),
        *shared,
        held(spread),
        held(pick),
        back,
        owned,
        held(mine),
        held(gaps),
        held(side),
    )
    result = pl.pallas_call(
        late_kernel,
        out_shape=jax.ShapeDtypeStruct((72, 2, D), jnp.bfloat16),
        in_specs=[whole] * 16,
        out_specs=whole,
        compiler_params=pltpu.CompilerParams(vmem_limit_bytes=VMEM_LIMIT),
        name="late",
    )(held(other), *[held(x) for x in early], *shared, back, owned, held(woven))
    return result.reshape(WLA, WLO, 2, D).transpose(2, 0, 1, 3)


def solution(mesh):
    placed = (
        P("lev", "lat", "lon", None),
        P(),
        P(),
        P(),
        P(None, "lat", None, None),
        P(),
        P(),
        P(),
    )
    return jax.shard_map(
        per_device,
        mesh=mesh,
        in_specs=placed,
        out_specs=P("lev", "lat", "lon", None),
        check_vma=False,
    )
```

```python
import numpy as np
import jax
import jax.numpy as jnp
from jax import lax
from jax.experimental import pallas as pl
from jax.experimental.pallas import tpu as pltpu
from jax.sharding import PartitionSpec as P

D = 192
HEADS = 6
HEAD_DIM = 32
WLA = 6
WLO = 12
HLA = 3
HLO = 6
SPAN = 2 * WLO - 1
ROWS = 288
HALF = 144
QROWS = 288
GROUP = 24
FAR = -1e30
LANES = 256
TABLE = 54
CELLS = 144
FAR_COLUMNS = 6
VMEM_LIMIT = 16 * 1024 * 1024

norm_eps = 1e-05


def constants():
    pick = np.zeros((2, QROWS, HALF), np.float32)
    back = np.zeros((72, 2 * QROWS), np.float32)
    owned = np.zeros((QROWS, D), np.float32)
    mine = np.zeros((72, ROWS), np.float32)
    for o in range(WLO):
        for a in range(WLA):
            mine[a * WLO + o, (HLA + a) * 24 + HLO + o] = 1
        for h in range(HEADS):
            for a in range(4):
                row = o * GROUP + h * 4 + a
                owned[row, h * HEAD_DIM : (h + 1) * HEAD_DIM] = 1
                if a < HLA:
                    pick[0, row, (HLA + a) * 24 + HLO + o] = 1
                    pick[1, row, a * 24 + HLO + o] = 1
                    back[a * WLO + o, row] = 1
                    back[(HLA + a) * WLO + o, QROWS + row] = 1
    gaps = np.zeros((3 * GROUP, TABLE), np.float32)
    for e in range(3):
        for h in range(HEADS):
            for a in range(HLA):
                gaps[e * GROUP + h * 4 + a, (e * HLA + a) * HEADS + h] = 1
    woven = np.zeros((2, 144, 72), np.float32)
    cell = np.arange(72)
    for at in range(2):
        woven[at, 2 * cell + at, cell] = 1
    bank = np.zeros((688, 768), np.float32)
    bank[:ROWS, :HALF] = pick[0]
    bank[:ROWS, 256 : 256 + HALF] = pick[1]
    bank[:ROWS, 512 : 512 + D] = owned
    bank[288:360, : 2 * QROWS] = back
    bank[368:440, :ROWS] = mine
    bank[368:440, 384 : 384 + TABLE] = gaps
    bank[448:592, :72] = woven[0]
    bank[448:592, 128:200] = woven[1]
    return bank


def counted(shape, dim):
    return lax.broadcasted_iota(jnp.int32, shape, dim)


def by_24(n):
    quotient = (n * 2731) >> 16
    return quotient, n - 24 * quotient


def one_hot(target, width):
    shape = (target.shape[0], width)
    return halved(jnp.where(counted(shape, 1) == target, 1.0, 0.0))


def normalized(values, gain):
    average = jnp.mean(values, axis=-1, keepdims=True)
    centered = values - average
    variance = jnp.mean(centered * centered, axis=-1, keepdims=True)
    return centered * lax.rsqrt(variance + norm_eps) * gain


def dot(a, b):
    return jnp.dot(a, b, preferred_element_type=jnp.float32)


def dot_t(a, b):
    return lax.dot_general(a, b, (((1,), (1,)), ((), ())), preferred_element_type=jnp.float32)


def halved(x):
    return x.astype(jnp.bfloat16)


def softmax_context(scores, values, owned):
    top = jnp.max(scores[0], axis=-1, keepdims=True)
    for s in scores[1:]:
        top = jnp.maximum(top, jnp.max(s, axis=-1, keepdims=True))
    weights = [jnp.exp(s - top) for s in scores]
    total = jnp.sum(weights[0], axis=-1, keepdims=True)
    for w in weights[1:]:
        total = total + jnp.sum(w, axis=-1, keepdims=True)
    inverse = 1.0 / total
    context = 0.0
    for w, v in zip(weights, values):
        context = context + dot(halved(w * inverse), v)
    return halved(context) * owned


def finish(own, parts, back, proj, gain, fc1, fc2_t):
    context = halved(dot(back, jnp.concatenate(parts, axis=0)))
    first = own + dot(context, proj)
    mixed = dot(halved(normalized(first, gain)), fc1)
    hidden = halved(mixed * (1.0 + lax.erf(mixed * (0.5**0.5))) * 0.5)
    return halved(first + dot_t(hidden, fc2_t))


def fetch_kernel(cells_ref, tables_ref, half_ref, own_ref, held_ref, sems):
    odd = lax.axis_index("lon") % 2
    copies = [
        pltpu.make_async_copy(cells_ref.at[:, pl.ds(HLO * odd, HLO)], half_ref, sems.at[0]),
        pltpu.make_async_copy(cells_ref, own_ref, sems.at[1]),
        pltpu.make_async_copy(tables_ref, held_ref, sems.at[2]),
    ]
    for copy in copies:
        copy.start()
    for copy in copies:
        copy.wait()


def pack_kernel(
    far_ref, joint_ref, tables_ref,
    wide_ref, lower_ref, sent_far_ref, sent_near_ref,
):
    lev = lax.axis_index("lev")
    lat_even = lax.axis_index("lat") % 2 == 0
    odd = lax.axis_index("lon") % 2
    joint = joint_ref[...].reshape(ROWS, D)
    far = far_ref[...].reshape(2 * WLA * FAR_COLUMNS, D)
    row = counted((ROWS, 1), 0)
    level = (row >= HALF).astype(jnp.int32)
    cell = row - HALF * level
    lat_row, column = by_24(cell)
    from_far = odd * (column - WLO - HLO) + (1 - odd) * (HLO - 1 - column) >= 0
    near_cell = cell + HLO * (2 * odd - 1)
    far_cell = lat_row * FAR_COLUMNS + column
    far_cell = far_cell + (1 - odd) * (FAR_COLUMNS - HLO) - odd * (WLO + HLO)
    near_pick = one_hot(jnp.where(from_far, -1, 2 * near_cell + level), ROWS)
    far_pick = one_hot(jnp.where(from_far, 2 * far_cell + level, -1), 2 * WLA * FAR_COLUMNS)
    wide = dot(near_pick, joint) + dot(far_pick, far)
    wide_ref[...] = halved(wide)
    head = jnp.concatenate([wide[:72], wide[HALF : HALF + 72]], axis=0)
    tail = jnp.concatenate([wide[72:HALF], wide[HALF + 72 :]], axis=0)

    tables = tables_ref[...].reshape(2 * HEADS, 4 * WLA * WLA * SPAN)
    kinds = [dot(one_hot(2 * counted((8, 1), 0) + i, 2 * HEADS), tables) for i in range(2)]
    width = WLA * WLA * SPAN
    part = lambda i, at: kinds[i][:HEADS, at * width : (at + 1) * width]
    entries = [
        jnp.where(lev == 0, part(1, 3), part(1, 0)),
        jnp.where(lev == 0, part(0, 0), part(0, 3)),
        jnp.where(lev == 0, part(0, 1), part(0, 2)),
    ]
    span = WLA * SPAN
    rows = [
        jnp.concatenate(
            [e[:, (at + a) * span : (at + a + 1) * span] for e in entries for a in range(HLA)],
            axis=0,
        )
        for at in (0, HLA)
    ]
    lower_ref[...] = halved(rows[0])
    blank = jnp.zeros((CELLS + TABLE, LANES), jnp.bfloat16)
    sent_far_ref[...] = blank
    sent_near_ref[...] = blank
    sent_far_ref[:CELLS, :D] = halved(jnp.where(lat_even, head, tail))
    sent_near_ref[:CELLS, :D] = halved(jnp.where(lat_even, tail, head))
    sent_far_ref[CELLS:, :span] = halved(rows[1])
    sent_near_ref[CELLS:, :span] = halved(rows[1])


def early_kernel(
    wide_ref,
    before_ref,
    lower_ref,
    gain1_ref,
    qkv_ref,
    proj_ref,
    gain2_ref,
    fc1_ref,
    fc2_ref,
    bank_ref,
    alone_ref,
    own_ref,
    asked_ref,
    value_ref,
    score_ref,
    bias_ref,
):
    lev = lax.axis_index("lev")
    lat = lax.axis_index("lat")
    lat_last = lax.axis_size("lat") - 1
    gain1 = gain1_ref[...]
    w_q = qkv_ref[:, :D]
    w_k = qkv_ref[:, D : 2 * D]
    w_v = qkv_ref[:, 2 * D :]
    owned = bank_ref[:ROWS, 512 : 512 + D]
    picks = [bank_ref[:ROWS, :HALF], bank_ref[:ROWS, 256 : 256 + HALF]]
    back = bank_ref[288:360, : 2 * QROWS]
    mine = bank_ref[368:440, :ROWS]
    gaps = bank_ref[368:440, 384 : 384 + TABLE]
    span = WLA * SPAN
    table = halved(
        jnp.concatenate(
            [
                dot(gaps, before_ref[CELLS:, :span]),
                dot(gaps, lower_ref[...]),
            ],
            axis=0,
        )
    )
    lat_place, column = by_24(counted((span, HALF), 1))
    offset = counted((span, HALF), 0) - (lat_place * SPAN + 17 - column)
    sides = [jnp.where(column < WLO, offset, -1), jnp.where(column < WLO, -1, offset)]
    spreads = []
    for o in range(WLO):
        chosen = jnp.where(sides[o >= HLO] == o, 1.0, 0.0)
        spreads.append(dot(table, halved(chosen)))
    row_half = counted((QROWS, HALF), 0) >= QROWS // 2
    lane = counted((QROWS, HALF), 1)
    same_side = row_half == (by_24(lane)[1] >= WLO)
    allowed = [
        same_side & ((lane >= 72) | (lat > 0)),
        same_side & ((lane < 72) | (lat < lat_last)),
    ]

    def bias_of(lat_window, entry):
        at = (lat_window * 3 + entry) * GROUP
        terms = jnp.concatenate([s[at : at + GROUP] for s in spreads], axis=0)
        return jnp.where(allowed[lat_window], terms, FAR)

    def asked_of(cells):
        n = halved(normalized(cells.astype(jnp.float32), gain1))
        queries = halved(dot(n, w_q))
        keys = halved(dot(n, w_k))
        values = halved(dot(n, w_v))
        out = []
        for lat_window in range(2):
            rows = slice(lat_window * HALF, (lat_window + 1) * HALF)
            asked = halved(dot(picks[lat_window], queries[rows])) * owned
            out.append((asked, dot_t(asked, keys[rows]) * HEAD_DIM**-0.5, values[rows]))
        return out

    pair_cells = wide_ref[1 - lev]
    for lat_window, (asked, scores, values) in enumerate(asked_of(pair_cells)):
        asked_ref[lat_window] = asked
        value_ref[lat_window] = values
        score_ref[lat_window] = scores + bias_of(lat_window, 1)
        bias_ref[lat_window] = bias_of(lat_window, 2)
    own_ref[...] = dot(mine, pair_cells)

    alone_cells = wide_ref[lev]
    parts = []
    for lat_window, (asked, scores, values) in enumerate(asked_of(alone_cells)):
        parts.append(softmax_context([scores + bias_of(lat_window, 0)], [values], owned))
    alone_ref[...] = finish(
        dot(mine, alone_cells),
        parts,
        back,
        proj_ref[...],
        gain2_ref[...],
        fc1_ref[...],
        fc2_ref[...],
    )


def late_kernel(
    other_ref,
    alone_ref,
    own_ref,
    asked_ref,
    value_ref,
    score_ref,
    bias_ref,
    gain1_ref,
    qkv_ref,
    proj_ref,
    gain2_ref,
    fc1_ref,
    fc2_ref,
    bank_ref,
    out_ref,
):
    lev = lax.axis_index("lev")
    owned = bank_ref[:ROWS, 512 : 512 + D]
    n = halved(normalized(other_ref[...].astype(jnp.float32), gain1_ref[...]))
    keys = halved(dot(n, qkv_ref[:, D : 2 * D]))
    values = halved(dot(n, qkv_ref[:, 2 * D :]))
    parts = []
    for lat_window in range(2):
        rows = slice(lat_window * HALF, (lat_window + 1) * HALF)
        scores = dot_t(asked_ref[lat_window], keys[rows]) * HEAD_DIM**-0.5 + bias_ref[lat_window]
        parts.append(
            softmax_context(
                [score_ref[lat_window], scores], [value_ref[lat_window], values[rows]], owned
            )
        )
    pair = finish(
        own_ref[...],
        parts,
        bank_ref[288:360, : 2 * QROWS],
        proj_ref[...],
        gain2_ref[...],
        fc1_ref[...],
        fc2_ref[...],
    )
    alone = alone_ref[...]
    lower = jnp.where(lev == 0, alone, pair)
    upper = jnp.where(lev == 0, pair, alone)
    result = halved(dot(bank_ref[448:592, :72], lower) + dot(bank_ref[448:592, 128:200], upper))
    out_ref[...] = result.reshape(72, 2, D)


def pairs_of(size, crossed):
    shift = 1 if crossed else 0
    return [[(2 * i + shift) % size, (2 * i + 1 + shift) % size] for i in range(size // 2)]


def swapped(block, axis, crossed):
    route = []
    for a, b in pairs_of(lax.axis_size(axis), crossed):
        route += [(a, b), (b, a)]
    return lax.ppermute(block, axis, route)


def per_device(
    tokens, norm1_gain, qkv_weight, proj_weight, earth_bias, norm2_gain, fc1_weight, fc2_weight
):
    lev = lax.axis_index("lev")
    lat = lax.axis_index("lat")
    lon_size = lax.axis_size("lon")
    lat_size = lax.axis_size("lat")
    lon_even = lax.axis_index("lon") % 2 == 0
    lat_even = lat % 2 == 0

    cells_t = tokens.transpose(1, 2, 0, 3)
    tables_t = earth_bias[:, 0].transpose(1, 0, 2)
    params = pltpu.CompilerParams(vmem_limit_bytes=VMEM_LIMIT)
    anywhere = pl.BlockSpec(memory_space=pltpu.HBM)
    half_t, own_t, tables_t = pl.pallas_call(
        fetch_kernel,
        out_shape=[
            pltpu.VMEM((WLA, HLO, 2, D), jnp.bfloat16),
            pltpu.VMEM(cells_t.shape, jnp.bfloat16),
            pltpu.VMEM(tables_t.shape, jnp.bfloat16),
        ],
        in_specs=[anywhere] * 2,
        out_specs=[pl.BlockSpec(memory_space=pltpu.VMEM)] * 3,
        scratch_shapes=[pltpu.SemaphoreType.DMA((3,))],
        compiler_params=params,
        name="fetch",
    )(*[pltpu.with_memory_space_constraint(x, pltpu.HBM) for x in (cells_t, tables_t)])
    far = swapped(half_t, "lon", True)
    joint = lax.all_gather(
        own_t, "lon", axis_index_groups=pairs_of(lon_size, False), axis=1, tiled=True
    )
    bank = jnp.asarray(constants(), jnp.bfloat16)
    whole = pl.BlockSpec(memory_space=pltpu.VMEM)
    held = lambda x: pltpu.with_memory_space_constraint(x, pltpu.VMEM)
    sent = pltpu.VMEM((CELLS + TABLE, LANES), jnp.bfloat16)
    wide, lower, sent_far, sent_near = pl.pallas_call(
        pack_kernel,
        out_shape=[
            pltpu.VMEM((ROWS, D), jnp.bfloat16),
            pltpu.VMEM((TABLE, WLA * SPAN), jnp.bfloat16),
            sent,
            sent,
        ],
        in_specs=[whole] * 3,
        out_specs=[whole] * 4,
        compiler_params=params,
        name="pack",
    )(
        held(far),
        held(joint),
        held(tables_t),
    )
    cells = CELLS
    lat_far = swapped(sent_far, "lat", True)
    lat_both = lax.all_gather(sent_near, "lat", axis_index_groups=pairs_of(lat_size, False))
    lat_near = jnp.where(lat_even, lat_both[1], lat_both[0])
    before = jnp.where(lat_even, lat_far, lat_near)
    after = jnp.where(lat_even, lat_near, lat_far)
    edges = (2, HLA * 24, D)
    extended = jnp.concatenate(
        [
            before[:cells, :D].reshape(edges),
            wide.reshape(2, HALF, D),
            after[:cells, :D].reshape(edges),
        ],
        axis=1,
    )
    other = swapped(lax.dynamic_index_in_dim(extended, 1 - lev, 0, False), "lev", False)

    shared = [
        held(a)
        for a in (
            norm1_gain.reshape(1, D),
            qkv_weight,
            proj_weight,
            norm2_gain.reshape(1, D),
            fc1_weight,
            fc2_weight.T,
        )
    ]
    bank = held(bank)
    passed = [
        pltpu.VMEM((72, D), jnp.bfloat16),
        pltpu.VMEM((72, D), jnp.float32),
        pltpu.VMEM((2, QROWS, D), jnp.bfloat16),
        pltpu.VMEM((2, HALF, D), jnp.bfloat16),
        pltpu.VMEM((2, QROWS, HALF), jnp.float32),
        pltpu.VMEM((2, QROWS, HALF), jnp.float32),
    ]
    early = pl.pallas_call(
        early_kernel,
        out_shape=passed,
        in_specs=[whole] * 10,
        out_specs=[whole] * 6,
        cost_estimate=pl.CostEstimate(flops=4_000_000_000, transcendentals=0, bytes_accessed=0),
        compiler_params=params,
        name="early",
    )(
        held(extended),
        held(before),
        held(lower),
        *shared,
        bank,
    )
    result = pl.pallas_call(
        late_kernel,
        out_shape=jax.ShapeDtypeStruct((72, 2, D), jnp.bfloat16),
        in_specs=[whole] * 14,
        out_specs=whole,
        compiler_params=params,
        name="late",
    )(held(other), *[held(x) for x in early], *shared, bank)
    return result.reshape(WLA, WLO, 2, D).transpose(2, 0, 1, 3)


def solution(mesh):
    placed = (
        P("lev", "lat", "lon", None),
        P(),
        P(),
        P(),
        P(None, "lat", None, None),
        P(),
        P(),
        P(),
    )
    return jax.shard_map(
        per_device,
        mesh=mesh,
        in_specs=placed,
        out_specs=P("lev", "lat", "lon", None),
        check_vma=False,
    )
```

```python
import jax
import jax.numpy as jnp
from jax import lax
from jax.experimental import pallas as pl
from jax.experimental.pallas import tpu as pltpu
from jax.sharding import PartitionSpec as P

D = 192
HEADS = 6
HEAD_DIM = 32
WLA = 6
WLO = 12
HLA = 3
HLO = 6
SPAN = 2 * WLO - 1
ROWS = 288
HALF = 144
QROWS = 216
GROUP = 18
FAR = -1e30
LANES = 256
TABLE = 54
CELLS = 144
FAR_COLUMNS = 6
VMEM_LIMIT = 16 * 1024 * 1024

norm_eps = 1e-05


def counted(shape, dim):
    return lax.broadcasted_iota(jnp.int32, shape, dim)


def by_24(n):
    quotient = (n * 2731) >> 16
    return quotient, n - 24 * quotient


def by_18(n):
    quotient = (n * 3641) >> 16
    return quotient, n - 18 * quotient


def by_3(n):
    quotient = (n * 21846) >> 16
    return quotient, n - 3 * quotient


def one_hot(target, width):
    shape = (target.shape[0], width)
    return halved(jnp.where(counted(shape, 1) == target, 1.0, 0.0))


def normalized(values, gain):
    average = jnp.mean(values, axis=-1, keepdims=True)
    centered = values - average
    variance = jnp.mean(centered * centered, axis=-1, keepdims=True)
    return centered * lax.rsqrt(variance + norm_eps) * gain


def dot(a, b):
    return jnp.dot(a, b, preferred_element_type=jnp.float32)


def dot_t(a, b):
    return lax.dot_general(a, b, (((1,), (1,)), ((), ())), preferred_element_type=jnp.float32)


def halved(x):
    return x.astype(jnp.bfloat16)


def softmax_context(scores, values, owned):
    top = jnp.max(scores[0], axis=-1, keepdims=True)
    for s in scores[1:]:
        top = jnp.maximum(top, jnp.max(s, axis=-1, keepdims=True))
    weights = [jnp.exp(s - top) for s in scores]
    total = jnp.sum(weights[0], axis=-1, keepdims=True)
    for w in weights[1:]:
        total = total + jnp.sum(w, axis=-1, keepdims=True)
    inverse = 1.0 / total
    context = 0.0
    for w, v in zip(weights, values):
        context = context + dot(halved(w * inverse), v)
    return halved(context) * owned


def finish(own, parts, back, proj, gain, fc1, fc2_t):
    context = halved(dot(back[0], parts[0]) + dot(back[1], parts[1]))
    first = own + dot(context, proj)
    mixed = dot(halved(normalized(first, gain)), fc1)
    hidden = halved(mixed * (1.0 + lax.erf(mixed * (0.5**0.5))) * 0.5)
    return halved(first + dot_t(hidden, fc2_t))


def fetch_kernel(
    cells_ref, tables_ref, gain1_ref, gain2_ref,
    half_ref, own_ref, rows_ref, held_ref, gain2_held, raw_ref, gain1_held, sems,
):
    odd = lax.axis_index("lon") % 2
    copies = [
        pltpu.make_async_copy(gain1_ref, gain1_held, sems.at[0]),
        pltpu.make_async_copy(cells_ref, raw_ref, sems.at[1]),
        pltpu.make_async_copy(tables_ref, held_ref, sems.at[2]),
        pltpu.make_async_copy(gain2_ref, gain2_held, sems.at[3]),
    ]
    for copy in copies:
        copy.start()
    copies[0].wait()
    copies[1].wait()
    rows = raw_ref[...].reshape(CELLS, D)
    rows_ref[...] = rows
    cells = rows.astype(jnp.float32)
    own_ref[...] = halved(normalized(cells, gain1_held[...])).reshape(raw_ref.shape)
    half_ref[...] = own_ref[:, pl.ds(HLO * odd, HLO)]
    copies[2].wait()
    copies[3].wait()


def pack_kernel(
    far_ref, joint_ref, tables_ref,
    wide_ref, lower_ref, sent_far_ref, sent_near_ref,
):
    lev = lax.axis_index("lev")
    lat_even = lax.axis_index("lat") % 2 == 0
    odd = lax.axis_index("lon") % 2
    joint = joint_ref[...].reshape(ROWS, D)
    far = far_ref[...].reshape(2 * WLA * FAR_COLUMNS, D)
    row = counted((ROWS, 1), 0)
    level = (row >= HALF).astype(jnp.int32)
    cell = row - HALF * level
    lat_row, column = by_24(cell)
    from_far = odd * (column - WLO - HLO) + (1 - odd) * (HLO - 1 - column) >= 0
    near_cell = cell + HLO * (2 * odd - 1)
    far_cell = lat_row * FAR_COLUMNS + column
    far_cell = far_cell + (1 - odd) * (FAR_COLUMNS - HLO) - odd * (WLO + HLO)
    near_pick = one_hot(jnp.where(from_far, -1, 2 * near_cell + level), ROWS)
    far_pick = one_hot(jnp.where(from_far, 2 * far_cell + level, -1), 2 * WLA * FAR_COLUMNS)
    wide = dot(near_pick, joint) + dot(far_pick, far)
    wide_ref[...] = halved(wide)
    head = jnp.concatenate([wide[:72], wide[HALF : HALF + 72]], axis=0)
    tail = jnp.concatenate([wide[72:HALF], wide[HALF + 72 :]], axis=0)

    tables = tables_ref[...].reshape(2 * HEADS, 4 * WLA * WLA * SPAN)
    kinds = [dot(one_hot(2 * counted((8, 1), 0) + i, 2 * HEADS), tables) for i in range(2)]
    width = WLA * WLA * SPAN
    part = lambda i, at: kinds[i][:HEADS, at * width : (at + 1) * width]
    entries = [
        jnp.where(lev == 0, part(1, 3), part(1, 0)),
        jnp.where(lev == 0, part(0, 0), part(0, 3)),
        jnp.where(lev == 0, part(0, 1), part(0, 2)),
    ]
    span = WLA * SPAN
    rows = [
        jnp.concatenate(
            [e[:, (at + a) * span : (at + a + 1) * span] for e in entries for a in range(HLA)],
            axis=0,
        )
        for at in (0, HLA)
    ]
    lower_ref[...] = halved(rows[0])
    blank = jnp.zeros((CELLS + TABLE, LANES), jnp.bfloat16)
    sent_far_ref[...] = blank
    sent_near_ref[...] = blank
    sent_far_ref[:CELLS, :D] = halved(jnp.where(lat_even, head, tail))
    sent_near_ref[:CELLS, :D] = halved(jnp.where(lat_even, tail, head))
    sent_far_ref[CELLS:, :span] = halved(rows[1])
    sent_near_ref[CELLS:, :span] = halved(rows[1])


def assemble_kernel(
    far_ref, both_ref, wide_ref, alone_ref, pair_ref, table_ref, sent_ref
):
    lev = lax.axis_index("lev")
    lat_odd = lax.axis_index("lat") % 2
    near = both_ref[1 - lat_odd].astype(jnp.float32)
    far = far_ref[...].astype(jnp.float32)
    wide = wide_ref[...].astype(jnp.float32)
    before = jnp.where(lat_odd == 0, far, near)
    after = jnp.where(lat_odd == 0, near, far)
    levels = [
        jnp.concatenate(
            [
                before[l * 72 : (l + 1) * 72, :D],
                wide[l * HALF : (l + 1) * HALF],
                after[l * 72 : (l + 1) * 72, :D],
            ],
            axis=0,
        )
        for l in range(2)
    ]
    pair = jnp.where(lev == 0, levels[1], levels[0])
    pair_ref[...] = halved(pair)
    first = pair[:HALF]
    second = pair[HALF:]
    sent_ref[:HALF] = halved(jnp.concatenate([first, second[:, : LANES - D]], axis=1))
    rest = second[:, LANES - D :]
    sent_ref[HALF:] = halved(jnp.concatenate([rest[:72], rest[72:]], axis=1))
    alone_ref[...] = halved(jnp.where(lev == 0, levels[0], levels[1]))
    table_ref[...] = halved(before[CELLS:, : WLA * SPAN])


def packed_dots(packed, weight):
    spare = jnp.zeros((LANES - D, weight.shape[1]), weight.dtype)
    first = dot(packed[:HALF], jnp.concatenate([weight, spare], axis=0))
    low = jnp.concatenate([spare, weight[: LANES - D]], axis=0)
    second = dot(packed[:HALF, LANES // 2 :], low)
    high = weight[LANES - D :]
    rest = [dot(packed[HALF:, : LANES // 2], high), dot(packed[HALF:, LANES // 2 :], high)]
    return halved(first), halved(second + jnp.concatenate(rest, axis=0))


def early_kernel(
    alone_cells_ref,
    pair_cells_ref,
    raw_ref,
    upper_ref,
    lower_ref,
    qkv_ref,
    proj_ref,
    fc1_ref,
    fc2_ref,
    gain2_ref,
    alone_ref,
    own_ref,
    asked_ref,
    value_ref,
    score_ref,
    bias_ref,
    owned_ref,
    back_ref,
    woven_ref,
):
    lev = lax.axis_index("lev")
    lat = lax.axis_index("lat")
    lat_last = lax.axis_size("lat") - 1
    column, spot = by_18(counted((QROWS, 1), 0))
    head, place = by_3(spot)
    picks = [one_hot((at + place) * 24 + HLO + column, HALF) for at in (HLA, 0)]
    owned = halved(jnp.where(counted((QROWS, D), 1) >> 5 == head, 1.0, 0.0))
    owned_ref[...] = owned
    column, spot = by_18(counted((1, QROWS), 1))
    source = by_3(spot)[1] * WLO + column
    cell = counted((72, QROWS), 0)
    back = [halved(jnp.where(cell == source + at * WLO, 1.0, 0.0)) for at in (0, HLA)]
    for at in range(2):
        back_ref[at] = back[at]
    raw = raw_ref[...]
    cell = 2 * counted((72, 1), 0)
    own_ref[...] = dot(one_hot(cell + 1 - lev, CELLS), raw)
    alone_own = dot(one_hot(cell + lev, CELLS), raw)
    woven_row = counted((CELLS, 72), 0) - 2 * counted((CELLS, 72), 1)
    woven_ref[...] = halved(jnp.where(woven_row == 1 - lev, 1.0, 0.0))
    entry, spot = by_18(counted((3 * GROUP, 1), 0))
    head, place = by_3(spot)
    gaps = one_hot((entry * HLA + place) * HEADS + head, TABLE)
    span = WLA * SPAN
    tables = [halved(dot(gaps, ref[...])) for ref in (upper_ref, lower_ref)]
    lat_place, column = by_24(counted((span, HALF), 1))
    offset = counted((span, HALF), 0) - (lat_place * SPAN + 17 - column)
    sides = [jnp.where(column < WLO, offset, -1), jnp.where(column < WLO, -1, offset)]
    spreads = []
    for o in range(WLO):
        chosen = jnp.where(sides[o >= HLO] == o, 1.0, 0.0)
        spreads.append([dot(table, halved(chosen)) for table in tables])
    row_half = counted((QROWS, HALF), 0) >= QROWS // 2
    lane = counted((QROWS, HALF), 1)
    same_side = row_half == (by_24(lane)[1] >= WLO)
    allowed = [
        same_side & ((lane >= 72) | (lat > 0)),
        same_side & ((lane < 72) | (lat < lat_last)),
    ]

    def bias_of(lat_window, entry):
        at = entry * GROUP
        terms = jnp.concatenate([s[lat_window][at : at + GROUP] for s in spreads], axis=0)
        return jnp.where(allowed[lat_window], terms, FAR)

    w_q = qkv_ref[:, :D]
    w_k = qkv_ref[:, D : 2 * D]
    w_v = qkv_ref[:, 2 * D :]

    def asked_of(n):
        queries = halved(dot(n, w_q))
        keys = halved(dot(n, w_k))
        values = halved(dot(n, w_v))
        out = []
        for lat_window in range(2):
            rows = slice(lat_window * HALF, (lat_window + 1) * HALF)
            asked = halved(dot(picks[lat_window], queries[rows])) * owned
            out.append((asked, dot_t(asked, keys[rows]) * HEAD_DIM**-0.5, values[rows]))
        return out

    for lat_window, (asked, scores, values) in enumerate(asked_of(pair_cells_ref[...])):
        asked_ref[lat_window] = asked
        value_ref[lat_window] = values
        score_ref[lat_window] = scores + bias_of(lat_window, 1)
        bias_ref[lat_window] = bias_of(lat_window, 2)

    parts = []
    for lat_window, (asked, scores, values) in enumerate(asked_of(alone_cells_ref[...])):
        parts.append(softmax_context([scores + bias_of(lat_window, 0)], [values], owned))
    alone = finish(
        alone_own,
        parts,
        back,
        proj_ref[...],
        gain2_ref[...],
        fc1_ref[...],
        fc2_ref[...],
    )
    alone_ref[...] = dot(halved(jnp.where(woven_row == lev, 1.0, 0.0)), alone)


def late_kernel(
    other_ref,
    alone_ref,
    own_ref,
    asked_ref,
    value_ref,
    score_ref,
    bias_ref,
    owned_ref,
    back_ref,
    woven_ref,
    qkv_ref,
    proj_ref,
    fc1_ref,
    fc2_ref,
    gain2_ref,
    out_ref,
):
    owned = owned_ref[...]
    packed = other_ref[...]
    keys = packed_dots(packed, qkv_ref[:, D : 2 * D])
    values = packed_dots(packed, qkv_ref[:, 2 * D :])
    parts = []
    for lat_window in range(2):
        scores = dot_t(asked_ref[lat_window], keys[lat_window]) * HEAD_DIM**-0.5 + bias_ref[lat_window]
        parts.append(
            softmax_context(
                [score_ref[lat_window], scores], [value_ref[lat_window], values[lat_window]], owned
            )
        )
    pair = finish(
        own_ref[...],
        parts,
        (back_ref[0], back_ref[1]),
        proj_ref[...],
        gain2_ref[...],
        fc1_ref[...],
        fc2_ref[...],
    )
    result = halved(alone_ref[...] + dot(woven_ref[...], pair))
    out_ref[...] = result.reshape(72, 2, D)


def pairs_of(size, crossed):
    shift = 1 if crossed else 0
    return [[(2 * i + shift) % size, (2 * i + 1 + shift) % size] for i in range(size // 2)]


def swapped(block, axis, crossed):
    route = []
    for a, b in pairs_of(lax.axis_size(axis), crossed):
        route += [(a, b), (b, a)]
    return lax.ppermute(block, axis, route)


def per_device(
    tokens, norm1_gain, qkv_weight, proj_weight, earth_bias, norm2_gain, fc1_weight, fc2_weight
):
    lon_size = lax.axis_size("lon")
    lat_size = lax.axis_size("lat")

    cells_t = tokens.transpose(1, 2, 0, 3)
    tables_t = earth_bias[:, 0].transpose(1, 0, 2)
    params = pltpu.CompilerParams(vmem_limit_bytes=VMEM_LIMIT)
    anywhere = pl.BlockSpec(memory_space=pltpu.HBM)
    half_t, own_t, raw_t, tables_t, gain2 = pl.pallas_call(
        fetch_kernel,
        out_shape=[
            pltpu.VMEM((WLA, HLO, 2, D), jnp.bfloat16),
            pltpu.VMEM(cells_t.shape, jnp.bfloat16),
            pltpu.VMEM((CELLS, D), jnp.bfloat16),
            pltpu.VMEM(tables_t.shape, jnp.bfloat16),
            pltpu.VMEM((1, D), jnp.float32),
        ],
        in_specs=[anywhere] * 4,
        out_specs=[pl.BlockSpec(memory_space=pltpu.VMEM)] * 5,
        scratch_shapes=[
            pltpu.VMEM(cells_t.shape, jnp.bfloat16),
            pltpu.VMEM((1, D), jnp.float32),
            pltpu.SemaphoreType.DMA((4,)),
        ],
        compiler_params=params,
        name="fetch",
    )(
        *[
            pltpu.with_memory_space_constraint(x, pltpu.HBM)
            for x in (
                cells_t,
                tables_t,
                norm1_gain.reshape(1, D),
                norm2_gain.reshape(1, D),
            )
        ]
    )
    far = swapped(half_t, "lon", True)
    joint = lax.all_gather(
        own_t, "lon", axis_index_groups=pairs_of(lon_size, False), axis=1, tiled=True
    )
    whole = pl.BlockSpec(memory_space=pltpu.VMEM)
    placed = pltpu.with_memory_space_constraint
    held = lambda x: placed(x, pltpu.VMEM)
    sent = pltpu.VMEM((CELLS + TABLE, LANES), jnp.bfloat16)
    wide, lower, sent_far, sent_near = pl.pallas_call(
        pack_kernel,
        out_shape=[
            pltpu.VMEM((ROWS, D), jnp.bfloat16),
            pltpu.VMEM((TABLE, WLA * SPAN), jnp.bfloat16),
            sent,
            sent,
        ],
        in_specs=[whole] * 3,
        out_specs=[whole] * 4,
        compiler_params=params,
        name="pack",
    )(
        held(far),
        held(joint),
        held(tables_t),
    )
    lat_far = swapped(sent_far, "lat", True)
    lat_both = lax.all_gather(sent_near, "lat", axis_index_groups=pairs_of(lat_size, False))
    level = pltpu.VMEM((ROWS, D), jnp.bfloat16)
    alone_cells, pair_cells, upper, sent = pl.pallas_call(
        assemble_kernel,
        out_shape=[
            level,
            level,
            pltpu.VMEM((TABLE, WLA * SPAN), jnp.bfloat16),
            pltpu.VMEM((HALF + 72, LANES), jnp.bfloat16),
        ],
        in_specs=[whole] * 3,
        out_specs=[whole] * 4,
        compiler_params=params,
        name="assemble",
    )(held(lat_far), held(lat_both), wide)
    other = swapped(sent, "lev", False)

    shared = (
        qkv_weight,
        proj_weight,
        fc1_weight,
        fc2_weight.T,
        gain2,
    )
    passed = [
        pltpu.VMEM((CELLS, D), jnp.float32),
        pltpu.VMEM((72, D), jnp.float32),
        pltpu.VMEM((2, QROWS, D), jnp.bfloat16),
        pltpu.VMEM((2, HALF, D), jnp.bfloat16),
        pltpu.VMEM((2, QROWS, HALF), jnp.float32),
        pltpu.VMEM((2, QROWS, HALF), jnp.float32),
        pltpu.VMEM((QROWS, D), jnp.bfloat16),
        pltpu.VMEM((2, 72, QROWS), jnp.bfloat16),
        pltpu.VMEM((CELLS, 72), jnp.bfloat16),
    ]
    shared = [held(x) for x in shared]
    early = pl.pallas_call(
        early_kernel,
        out_shape=passed,
        in_specs=[whole] * (5 + len(shared)),
        out_specs=[whole] * len(passed),
        cost_estimate=pl.CostEstimate(flops=4_000_000_000, transcendentals=0, bytes_accessed=0),
        compiler_params=params,
        name="early",
    )(alone_cells, pair_cells, raw_t, upper, lower, *shared)
    result = pl.pallas_call(
        late_kernel,
        out_shape=jax.ShapeDtypeStruct((72, 2, D), jnp.bfloat16),
        in_specs=[whole] * 15,
        out_specs=whole,
        compiler_params=params,
        name="late",
    )(held(other), *early, *shared)
    return result.reshape(WLA, WLO, 2, D).transpose(2, 0, 1, 3)


def solution(mesh):
    placed = (
        P("lev", "lat", "lon", None),
        P(),
        P(),
        P(),
        P(None, "lat", None, None),
        P(),
        P(),
        P(),
    )
    return jax.shard_map(
        per_device,
        mesh=mesh,
        in_specs=placed,
        out_specs=P("lev", "lat", "lon", None),
        check_vma=False,
    )
```

```python
import jax
import jax.numpy as jnp
from jax import lax
from jax.experimental import pallas as pl
from jax.experimental.pallas import tpu as pltpu
from jax.sharding import PartitionSpec as P

D = 192
HEADS = 6
HEAD_DIM = 32
WLA = 6
WLO = 12
HLA = 3
HLO = 6
SPAN = 2 * WLO - 1
ROWS = 288
HALF = 144
QROWS = 216
GROUP = 18
FAR = -1e30
LANES = 256
TABLE = 54
CELLS = 144
SENT = 112
FAR_COLUMNS = 12
VMEM_LIMIT = 16 * 1024 * 1024

norm_eps = 1e-05


def counted(shape, dim):
    return lax.broadcasted_iota(jnp.int32, shape, dim)


def by_24(n):
    quotient = (n * 2731) >> 16
    return quotient, n - 24 * quotient


def by_18(n):
    quotient = (n * 3641) >> 16
    return quotient, n - 18 * quotient


def by_3(n):
    quotient = (n * 21846) >> 16
    return quotient, n - 3 * quotient


def one_hot(target, width):
    shape = (target.shape[0], width)
    return halved(jnp.where(counted(shape, 1) == target, 1.0, 0.0))


def normalized(values, gain):
    average = jnp.mean(values, axis=-1, keepdims=True)
    centered = values - average
    variance = jnp.mean(centered * centered, axis=-1, keepdims=True)
    return centered * lax.rsqrt(variance + norm_eps) * gain


def dot(a, b):
    return jnp.dot(a, b, preferred_element_type=jnp.float32)


def dot_t(a, b):
    return lax.dot_general(a, b, (((1,), (1,)), ((), ())), preferred_element_type=jnp.float32)


def halved(x):
    return x.astype(jnp.bfloat16)


def softmax_context(scores, values, owned):
    top = jnp.max(scores[0], axis=-1, keepdims=True)
    for s in scores[1:]:
        top = jnp.maximum(top, jnp.max(s, axis=-1, keepdims=True))
    weights = [jnp.exp(s - top) for s in scores]
    total = jnp.sum(weights[0], axis=-1, keepdims=True)
    for w in weights[1:]:
        total = total + jnp.sum(w, axis=-1, keepdims=True)
    inverse = 1.0 / total
    context = 0.0
    for w, v in zip(weights, values):
        context = context + dot(halved(w * inverse), v)
    return halved(context) * owned


def finish(own, parts, back, proj, gain, fc1, fc2_t):
    context = halved(dot(back[0], parts[0]) + dot(back[1], parts[1]))
    first = own + dot(context, proj)
    mixed = dot(halved(normalized(first, gain)), fc1)
    hidden = halved(mixed * (1.0 + lax.erf(mixed * (0.5**0.5))) * 0.5)
    return halved(first + dot_t(hidden, fc2_t))


def pack_kernel(
    far_ref, joint_ref, tables_ref,
    wide_ref, lower_ref, sent_far_ref, sent_near_ref,
):
    lev = lax.axis_index("lev")
    lat_even = lax.axis_index("lat") % 2 == 0
    odd = lax.axis_index("lon") % 2
    joint = joint_ref[...].reshape(ROWS, D)
    far = far_ref[...].reshape(2 * WLA * FAR_COLUMNS, D)
    row = counted((ROWS, 1), 0)
    level = (row >= HALF).astype(jnp.int32)
    cell = row - HALF * level
    lat_row, column = by_24(cell)
    from_far = odd * (column - WLO - HLO) + (1 - odd) * (HLO - 1 - column) >= 0
    near_cell = cell + HLO * (2 * odd - 1)
    far_cell = lat_row * FAR_COLUMNS + column
    far_cell = far_cell + (1 - odd) * (FAR_COLUMNS - HLO) - odd * (WLO + HLO)
    near_pick = one_hot(jnp.where(from_far, -1, 2 * near_cell + level), ROWS)
    far_pick = one_hot(jnp.where(from_far, 2 * far_cell + level, -1), 2 * WLA * FAR_COLUMNS)
    wide = dot(near_pick, joint) + dot(far_pick, far)
    wide_ref[...] = halved(wide)
    head = jnp.concatenate([wide[:72], wide[HALF : HALF + 72]], axis=0)
    tail = jnp.concatenate([wide[72:HALF], wide[HALF + 72 :]], axis=0)

    tables = tables_ref[...].reshape(2 * HEADS, 4 * WLA * WLA * SPAN)
    kinds = [dot(one_hot(2 * counted((8, 1), 0) + i, 2 * HEADS), tables) for i in range(2)]
    width = WLA * WLA * SPAN
    part = lambda i, at: kinds[i][:HEADS, at * width : (at + 1) * width]
    entries = [
        jnp.where(lev == 0, part(1, 3), part(1, 0)),
        jnp.where(lev == 0, part(0, 0), part(0, 3)),
        jnp.where(lev == 0, part(0, 1), part(0, 2)),
    ]
    span = WLA * SPAN
    rows = [
        jnp.concatenate(
            [e[:, (at + a) * span : (at + a + 1) * span] for e in entries for a in range(HLA)],
            axis=0,
        )
        for at in (0, HLA)
    ]
    lower_ref[...] = halved(rows[0])
    upper = jnp.concatenate([rows[1], jnp.zeros((TABLE, LANES - span), jnp.float32)], axis=1)
    for ref, cells in (
        (sent_far_ref, jnp.where(lat_even, head, tail)),
        (sent_near_ref, jnp.where(lat_even, tail, head)),
    ):
        second = cells[72:]
        rest = second[:, LANES - D :]
        ref[:72] = halved(jnp.concatenate([cells[:72], second[:, : LANES - D]], axis=1))
        ref[72:SENT] = halved(jnp.concatenate([rest[:40], rest[32:]], axis=1))
        ref[SENT:] = halved(upper)


def assemble_kernel(
    far_ref, both_ref, wide_ref, gain_ref, gain2_ref, gain2_out, alone_ref, pair_ref, table_ref, sent_ref
):
    lev = lax.axis_index("lev")
    lat_odd = lax.axis_index("lat") % 2
    near = both_ref[1 - lat_odd].astype(jnp.float32)
    far = far_ref[...].astype(jnp.float32)
    wide = wide_ref[...].astype(jnp.float32)
    before = jnp.where(lat_odd == 0, far, near)
    after = jnp.where(lat_odd == 0, near, far)

    def unpacked(rows):
        rest = [rows[72:SENT, : LANES // 2], rows[80:SENT, LANES // 2 :]]
        second = [rows[:72, D:], jnp.concatenate(rest, axis=0)]
        return rows[:72, :D], jnp.concatenate(second, axis=1)

    edges = unpacked(before), unpacked(after)
    levels = [
        jnp.concatenate(
            [
                edges[0][l],
                wide[l * HALF : (l + 1) * HALF],
                edges[1][l],
            ],
            axis=0,
        )
        for l in range(2)
    ]
    gain2_out[...] = gain2_ref[...]
    pair = normalized(jnp.where(lev == 0, levels[1], levels[0]), gain_ref[...])
    pair_ref[...] = halved(pair)
    first = pair[:HALF]
    second = pair[HALF:]
    sent_ref[:HALF] = halved(jnp.concatenate([first, second[:, : LANES - D]], axis=1))
    rest = second[:, LANES - D :]
    sent_ref[HALF:] = halved(jnp.concatenate([rest[:72], rest[72:]], axis=1))
    alone_ref[...] = halved(jnp.where(lev == 0, levels[0], levels[1]))
    table_ref[...] = halved(before[SENT:, : WLA * SPAN])


def packed_dots(packed, weight):
    spare = jnp.zeros((LANES - D, weight.shape[1]), weight.dtype)
    first = dot(packed[:HALF], jnp.concatenate([weight, spare], axis=0))
    low = jnp.concatenate([spare, weight[: LANES - D]], axis=0)
    second = dot(packed[:HALF, LANES // 2 :], low)
    high = weight[LANES - D :]
    rest = [dot(packed[HALF:, : LANES // 2], high), dot(packed[HALF:, LANES // 2 :], high)]
    return halved(first), halved(second + jnp.concatenate(rest, axis=0))


def early_kernel(
    alone_cells_ref,
    pair_cells_ref,
    wide_ref,
    gain1_ref,
    upper_ref,
    lower_ref,
    qkv_ref,
    proj_ref,
    fc1_ref,
    fc2_ref,
    gain2_ref,
    alone_ref,
    own_ref,
    asked_ref,
    value_ref,
    score_ref,
    bias_ref,
    owned_ref,
    back_ref,
    woven_ref,
):
    lev = lax.axis_index("lev")
    lat = lax.axis_index("lat")
    lat_last = lax.axis_size("lat") - 1
    column, spot = by_18(counted((QROWS, 1), 0))
    head, place = by_3(spot)
    picks = [one_hot((at + place) * 24 + HLO + column, HALF) for at in (HLA, 0)]
    owned = halved(jnp.where(counted((QROWS, D), 1) >> 5 == head, 1.0, 0.0))
    owned_ref[...] = owned
    column, spot = by_18(counted((1, QROWS), 1))
    source = by_3(spot)[1] * WLO + column
    cell = counted((72, QROWS), 0)
    back = [halved(jnp.where(cell == source + at * WLO, 1.0, 0.0)) for at in (0, HLA)]
    for at in range(2):
        back_ref[at] = back[at]
    wide = wide_ref[...]
    place = counted((72, 1), 0)
    lat_row = (place * 5462) >> 16
    cell = lat_row * 24 + HLO + place - WLO * lat_row
    own_ref[...] = dot(one_hot(cell + HALF * (1 - lev), ROWS), wide)
    alone_own = dot(one_hot(cell + HALF * lev, ROWS), wide)
    woven_row = counted((CELLS, 72), 0) - 2 * counted((CELLS, 72), 1)
    woven_ref[...] = halved(jnp.where(woven_row == 1 - lev, 1.0, 0.0))
    entry, spot = by_18(counted((3 * GROUP, 1), 0))
    head, place = by_3(spot)
    gaps = one_hot((entry * HLA + place) * HEADS + head, TABLE)
    span = WLA * SPAN
    tables = [halved(dot(gaps, ref[...])) for ref in (upper_ref, lower_ref)]
    lat_place, column = by_24(counted((span, HALF), 1))
    offset = counted((span, HALF), 0) - (lat_place * SPAN + 17 - column)
    sides = [jnp.where(column < WLO, offset, -1), jnp.where(column < WLO, -1, offset)]
    spreads = []
    for o in range(WLO):
        chosen = jnp.where(sides[o >= HLO] == o, 1.0, 0.0)
        spreads.append([dot(table, halved(chosen)) for table in tables])
    row_half = counted((QROWS, HALF), 0) >= QROWS // 2
    lane = counted((QROWS, HALF), 1)
    same_side = row_half == (by_24(lane)[1] >= WLO)
    allowed = [
        same_side & ((lane >= 72) | (lat > 0)),
        same_side & ((lane < 72) | (lat < lat_last)),
    ]

    def bias_of(lat_window, entry):
        at = entry * GROUP
        terms = jnp.concatenate([s[lat_window][at : at + GROUP] for s in spreads], axis=0)
        return jnp.where(allowed[lat_window], terms, FAR)

    w_q = qkv_ref[:, :D]
    w_k = qkv_ref[:, D : 2 * D]
    w_v = qkv_ref[:, 2 * D :]

    def asked_of(n):
        queries = halved(dot(n, w_q))
        keys = halved(dot(n, w_k))
        values = halved(dot(n, w_v))
        out = []
        for lat_window in range(2):
            rows = slice(lat_window * HALF, (lat_window + 1) * HALF)
            asked = halved(dot(picks[lat_window], queries[rows])) * owned
            out.append((asked, dot_t(asked, keys[rows]) * HEAD_DIM**-0.5, values[rows]))
        return out

    for lat_window, (asked, scores, values) in enumerate(asked_of(pair_cells_ref[...])):
        asked_ref[lat_window] = asked
        value_ref[lat_window] = values
        score_ref[lat_window] = scores + bias_of(lat_window, 1)
        bias_ref[lat_window] = bias_of(lat_window, 2)

    parts = []
    for lat_window, (asked, scores, values) in enumerate(asked_of(halved(normalized(alone_cells_ref[...].astype(jnp.float32), gain1_ref[...])))):
        parts.append(softmax_context([scores + bias_of(lat_window, 0)], [values], owned))
    alone = finish(
        alone_own,
        parts,
        back,
        proj_ref[...],
        gain2_ref[...],
        fc1_ref[...],
        fc2_ref[...],
    )
    alone_ref[...] = dot(halved(jnp.where(woven_row == lev, 1.0, 0.0)), alone)


def late_kernel(
    other_ref,
    alone_ref,
    own_ref,
    asked_ref,
    value_ref,
    score_ref,
    bias_ref,
    owned_ref,
    back_ref,
    woven_ref,
    qkv_ref,
    proj_ref,
    fc1_ref,
    fc2_ref,
    gain2_ref,
    out_ref,
):
    owned = owned_ref[...]
    packed = other_ref[...]
    keys = packed_dots(packed, qkv_ref[:, D : 2 * D])
    values = packed_dots(packed, qkv_ref[:, 2 * D :])
    parts = []
    for lat_window in range(2):
        scores = dot_t(asked_ref[lat_window], keys[lat_window]) * HEAD_DIM**-0.5 + bias_ref[lat_window]
        parts.append(
            softmax_context(
                [score_ref[lat_window], scores], [value_ref[lat_window], values[lat_window]], owned
            )
        )
    pair = finish(
        own_ref[...],
        parts,
        (back_ref[0], back_ref[1]),
        proj_ref[...],
        gain2_ref[...],
        fc1_ref[...],
        fc2_ref[...],
    )
    result = halved(alone_ref[...] + dot(woven_ref[...], pair))
    out_ref[...] = result.reshape(72, 2, D)


def pairs_of(size, crossed):
    shift = 1 if crossed else 0
    return [[(2 * i + shift) % size, (2 * i + 1 + shift) % size] for i in range(size // 2)]


def swapped(block, axis, crossed):
    route = []
    for a, b in pairs_of(lax.axis_size(axis), crossed):
        route += [(a, b), (b, a)]
    return lax.ppermute(block, axis, route)


def per_device(
    tokens, norm1_gain, qkv_weight, proj_weight, earth_bias, norm2_gain, fc1_weight, fc2_weight
):
    lon_size = lax.axis_size("lon")
    lat_size = lax.axis_size("lat")

    cells_t = tokens.transpose(1, 2, 0, 3)
    tables_t = earth_bias[:, 0].transpose(1, 0, 2)
    params = pltpu.CompilerParams(vmem_limit_bytes=VMEM_LIMIT)
    far = swapped(cells_t, "lon", True)
    joint = lax.all_gather(
        cells_t, "lon", axis_index_groups=pairs_of(lon_size, False), axis=1, tiled=True
    )
    whole = pl.BlockSpec(memory_space=pltpu.VMEM)
    placed = pltpu.with_memory_space_constraint
    held = lambda x: placed(x, pltpu.VMEM)
    sent = pltpu.VMEM((SENT + TABLE, LANES), jnp.bfloat16)
    wide, lower, sent_far, sent_near = pl.pallas_call(
        pack_kernel,
        out_shape=[
            pltpu.VMEM((ROWS, D), jnp.bfloat16),
            pltpu.VMEM((TABLE, WLA * SPAN), jnp.bfloat16),
            sent,
            sent,
        ],
        in_specs=[whole] * 3,
        out_specs=[whole] * 4,
        compiler_params=params,
        name="pack",
    )(
        held(far),
        held(joint),
        held(tables_t),
    )
    lat_far = swapped(sent_far, "lat", True)
    lat_both = lax.all_gather(sent_near, "lat", axis_index_groups=pairs_of(lat_size, False))
    gain1 = held(norm1_gain.reshape(1, D))
    level = pltpu.VMEM((ROWS, D), jnp.bfloat16)
    gain2, alone_cells, pair_cells, upper, sent = pl.pallas_call(
        assemble_kernel,
        out_shape=[
            pltpu.VMEM((1, D), jnp.float32),
            level,
            level,
            pltpu.VMEM((TABLE, WLA * SPAN), jnp.bfloat16),
            pltpu.VMEM((HALF + 72, LANES), jnp.bfloat16),
        ],
        in_specs=[whole] * 5,
        out_specs=[whole] * 5,
        compiler_params=params,
        name="assemble",
    )(held(lat_far), held(lat_both), wide, gain1, held(norm2_gain.reshape(1, D)))
    other = swapped(sent, "lev", False)

    shared = (
        qkv_weight,
        proj_weight,
        fc1_weight,
        fc2_weight.T,
        gain2,
    )
    passed = [
        pltpu.VMEM((CELLS, D), jnp.float32),
        pltpu.VMEM((72, D), jnp.float32),
        pltpu.VMEM((2, QROWS, D), jnp.bfloat16),
        pltpu.VMEM((2, HALF, D), jnp.bfloat16),
        pltpu.VMEM((2, QROWS, HALF), jnp.float32),
        pltpu.VMEM((2, QROWS, HALF), jnp.float32),
        pltpu.VMEM((QROWS, D), jnp.bfloat16),
        pltpu.VMEM((2, 72, QROWS), jnp.bfloat16),
        pltpu.VMEM((CELLS, 72), jnp.bfloat16),
    ]
    shared = [held(x) for x in shared]
    early = pl.pallas_call(
        early_kernel,
        out_shape=passed,
        in_specs=[whole] * (6 + len(shared)),
        out_specs=[whole] * len(passed),
        cost_estimate=pl.CostEstimate(flops=4_000_000_000, transcendentals=0, bytes_accessed=0),
        compiler_params=params,
        name="early",
    )(alone_cells, pair_cells, wide, gain1, upper, lower, *shared)
    result = pl.pallas_call(
        late_kernel,
        out_shape=jax.ShapeDtypeStruct((72, 2, D), jnp.bfloat16),
        in_specs=[whole] * 15,
        out_specs=whole,
        compiler_params=params,
        name="late",
    )(held(other), *early, *shared)
    return result.reshape(WLA, WLO, 2, D).transpose(2, 0, 1, 3)


def solution(mesh):
    placed = (
        P("lev", "lat", "lon", None),
        P(),
        P(),
        P(),
        P(None, "lat", None, None),
        P(),
        P(),
        P(),
    )
    return jax.shard_map(
        per_device,
        mesh=mesh,
        in_specs=placed,
        out_specs=P("lev", "lat", "lon", None),
        check_vma=False,
    )
```

```python
import jax
import jax.numpy as jnp
from jax import lax
from jax.experimental import pallas as pl
from jax.experimental.pallas import tpu as pltpu
from jax.sharding import PartitionSpec as P

D = 192
HEADS = 6
HEAD_DIM = 32
WLA = 6
WLO = 12
HLA = 3
HLO = 6
SPAN = 2 * WLO - 1
ROWS = 288
HALF = 144
QROWS = 216
GROUP = 18
FAR = -1e30
LANES = 256
TABLE = 54
CELLS = 144
SENT = 112
FAR_COLUMNS = 6
VMEM_LIMIT = 16 * 1024 * 1024

norm_eps = 1e-05


def counted(shape, dim):
    return lax.broadcasted_iota(jnp.int32, shape, dim)


def by_24(n):
    quotient = (n * 2731) >> 16
    return quotient, n - 24 * quotient


def by_18(n):
    quotient = (n * 3641) >> 16
    return quotient, n - 18 * quotient


def by_3(n):
    quotient = (n * 21846) >> 16
    return quotient, n - 3 * quotient


def one_hot(target, width):
    shape = (target.shape[0], width)
    return halved(jnp.where(counted(shape, 1) == target, 1.0, 0.0))


def normalized(values, gain):
    average = jnp.mean(values, axis=-1, keepdims=True)
    centered = values - average
    variance = jnp.mean(centered * centered, axis=-1, keepdims=True)
    return centered * lax.rsqrt(variance + norm_eps) * gain


def dot(a, b):
    return jnp.dot(a, b, preferred_element_type=jnp.float32)


def dot_t(a, b):
    return lax.dot_general(a, b, (((1,), (1,)), ((), ())), preferred_element_type=jnp.float32)


def halved(x):
    return x.astype(jnp.bfloat16)


def softmax_context(scores, values, owned):
    top = jnp.max(scores[0], axis=-1, keepdims=True)
    for s in scores[1:]:
        top = jnp.maximum(top, jnp.max(s, axis=-1, keepdims=True))
    weights = [jnp.exp(s - top) for s in scores]
    total = jnp.sum(weights[0], axis=-1, keepdims=True)
    for w in weights[1:]:
        total = total + jnp.sum(w, axis=-1, keepdims=True)
    inverse = 1.0 / total
    context = 0.0
    for w, v in zip(weights, values):
        context = context + dot(halved(w * inverse), v)
    return halved(context) * owned


def finish(own, parts, back, proj, gain, fc1, fc2_t):
    context = halved(dot(back[0], parts[0]) + dot(back[1], parts[1]))
    first = own + dot(context, proj)
    mixed = dot(halved(normalized(first, gain)), fc1)
    hidden = halved(mixed * (1.0 + lax.erf(mixed * (0.5**0.5))) * 0.5)
    return halved(first + dot_t(hidden, fc2_t))


def half_kernel(cells_ref, half_ref, sem):
    odd = lax.axis_index("lon") % 2
    copy = pltpu.make_async_copy(cells_ref.at[:, pl.ds(HLO * odd, HLO)], half_ref, sem)
    copy.start()
    copy.wait()


def pack_kernel(
    far_ref, joint_ref, tables_ref,
    wide_ref, lower_ref, sent_far_ref, sent_near_ref,
):
    lev = lax.axis_index("lev")
    lat_even = lax.axis_index("lat") % 2 == 0
    odd = lax.axis_index("lon") % 2
    joint = joint_ref[...].reshape(ROWS, D)
    far = far_ref[...].reshape(2 * WLA * FAR_COLUMNS, D)
    row = counted((ROWS, 1), 0)
    level = (row >= HALF).astype(jnp.int32)
    cell = row - HALF * level
    lat_row, column = by_24(cell)
    from_far = odd * (column - WLO - HLO) + (1 - odd) * (HLO - 1 - column) >= 0
    near_cell = cell + HLO * (2 * odd - 1)
    far_cell = lat_row * FAR_COLUMNS + column
    far_cell = far_cell + (1 - odd) * (FAR_COLUMNS - HLO) - odd * (WLO + HLO)
    near_pick = one_hot(jnp.where(from_far, -1, 2 * near_cell + level), ROWS)
    far_pick = one_hot(jnp.where(from_far, 2 * far_cell + level, -1), 2 * WLA * FAR_COLUMNS)
    wide = dot(near_pick, joint) + dot(far_pick, far)
    wide_ref[...] = halved(wide)
    head = jnp.concatenate([wide[:72], wide[HALF : HALF + 72]], axis=0)
    tail = jnp.concatenate([wide[72:HALF], wide[HALF + 72 :]], axis=0)

    tables = tables_ref[...].reshape(2 * HEADS, 4 * WLA * WLA * SPAN)
    kinds = [dot(one_hot(2 * counted((8, 1), 0) + i, 2 * HEADS), tables) for i in range(2)]
    width = WLA * WLA * SPAN
    part = lambda i, at: kinds[i][:HEADS, at * width : (at + 1) * width]
    entries = [
        jnp.where(lev == 0, part(1, 3), part(1, 0)),
        jnp.where(lev == 0, part(0, 0), part(0, 3)),
        jnp.where(lev == 0, part(0, 1), part(0, 2)),
    ]
    span = WLA * SPAN
    rows = [
        jnp.concatenate(
            [e[:, (at + a) * span : (at + a + 1) * span] for e in entries for a in range(HLA)],
            axis=0,
        )
        for at in (0, HLA)
    ]
    lower_ref[...] = halved(rows[0])
    upper = jnp.concatenate([rows[1], jnp.zeros((TABLE, LANES - span), jnp.float32)], axis=1)
    for ref, cells in (
        (sent_far_ref, jnp.where(lat_even, head, tail)),
        (sent_near_ref, jnp.where(lat_even, tail, head)),
    ):
        second = cells[72:]
        rest = second[:, LANES - D :]
        ref[:72] = halved(jnp.concatenate([cells[:72], second[:, : LANES - D]], axis=1))
        ref[72:SENT] = halved(jnp.concatenate([rest[:40], rest[32:]], axis=1))
        ref[SENT:] = halved(upper)


def assemble_kernel(
    far_ref, both_ref, wide_ref, gain_ref, gain2_ref, gain2_out, alone_ref, pair_ref, table_ref, sent_ref
):
    lev = lax.axis_index("lev")
    lat_odd = lax.axis_index("lat") % 2
    near = both_ref[1 - lat_odd].astype(jnp.float32)
    far = far_ref[...].astype(jnp.float32)
    wide = wide_ref[...].astype(jnp.float32)
    before = jnp.where(lat_odd == 0, far, near)
    after = jnp.where(lat_odd == 0, near, far)

    def unpacked(rows):
        rest = [rows[72:SENT, : LANES // 2], rows[80:SENT, LANES // 2 :]]
        second = [rows[:72, D:], jnp.concatenate(rest, axis=0)]
        return rows[:72, :D], jnp.concatenate(second, axis=1)

    edges = unpacked(before), unpacked(after)
    levels = [
        jnp.concatenate(
            [
                edges[0][l],
                wide[l * HALF : (l + 1) * HALF],
                edges[1][l],
            ],
            axis=0,
        )
        for l in range(2)
    ]
    gain2_out[...] = gain2_ref[...]
    pair = normalized(jnp.where(lev == 0, levels[1], levels[0]), gain_ref[...])
    pair_ref[...] = halved(pair)
    first = pair[:HALF]
    second = pair[HALF:]
    sent_ref[:HALF] = halved(jnp.concatenate([first, second[:, : LANES - D]], axis=1))
    rest = second[:, LANES - D :]
    sent_ref[HALF:] = halved(jnp.concatenate([rest[:72], rest[72:]], axis=1))
    alone_ref[...] = halved(jnp.where(lev == 0, levels[0], levels[1]))
    table_ref[...] = halved(before[SENT:, : WLA * SPAN])


def packed_dots(packed, weight):
    spare = jnp.zeros((LANES - D, weight.shape[1]), weight.dtype)
    first = dot(packed[:HALF], jnp.concatenate([weight, spare], axis=0))
    low = jnp.concatenate([spare, weight[: LANES - D]], axis=0)
    second = dot(packed[:HALF, LANES // 2 :], low)
    high = weight[LANES - D :]
    rest = [dot(packed[HALF:, : LANES // 2], high), dot(packed[HALF:, LANES // 2 :], high)]
    return halved(first), halved(second + jnp.concatenate(rest, axis=0))


def early_kernel(
    alone_cells_ref,
    pair_cells_ref,
    wide_ref,
    gain1_ref,
    upper_ref,
    lower_ref,
    qkv_ref,
    proj_ref,
    fc1_ref,
    fc2_ref,
    gain2_ref,
    alone_ref,
    own_ref,
    asked_ref,
    value_ref,
    score_ref,
    bias_ref,
    owned_ref,
    back_ref,
    woven_ref,
):
    lev = lax.axis_index("lev")
    lat = lax.axis_index("lat")
    lat_last = lax.axis_size("lat") - 1
    column, spot = by_18(counted((QROWS, 1), 0))
    head, place = by_3(spot)
    picks = [one_hot((at + place) * 24 + HLO + column, HALF) for at in (HLA, 0)]
    owned = halved(jnp.where(counted((QROWS, D), 1) >> 5 == head, 1.0, 0.0))
    owned_ref[...] = owned
    column, spot = by_18(counted((1, QROWS), 1))
    source = by_3(spot)[1] * WLO + column
    cell = counted((72, QROWS), 0)
    back = [halved(jnp.where(cell == source + at * WLO, 1.0, 0.0)) for at in (0, HLA)]
    for at in range(2):
        back_ref[at] = back[at]
    wide = wide_ref[...]
    place = counted((72, 1), 0)
    lat_row = (place * 5462) >> 16
    cell = lat_row * 24 + HLO + place - WLO * lat_row
    own_ref[...] = dot(one_hot(cell + HALF * (1 - lev), ROWS), wide)
    alone_own = dot(one_hot(cell + HALF * lev, ROWS), wide)
    woven_row = counted((CELLS, 72), 0) - 2 * counted((CELLS, 72), 1)
    woven_ref[...] = halved(jnp.where(woven_row == 1 - lev, 1.0, 0.0))
    entry, spot = by_18(counted((3 * GROUP, 1), 0))
    head, place = by_3(spot)
    gaps = one_hot((entry * HLA + place) * HEADS + head, TABLE)
    span = WLA * SPAN
    tables = [halved(dot(gaps, ref[...])) for ref in (upper_ref, lower_ref)]
    lat_place, column = by_24(counted((span, HALF), 1))
    offset = counted((span, HALF), 0) - (lat_place * SPAN + 17 - column)
    sides = [jnp.where(column < WLO, offset, -1), jnp.where(column < WLO, -1, offset)]
    spreads = []
    for o in range(WLO):
        chosen = jnp.where(sides[o >= HLO] == o, 1.0, 0.0)
        spreads.append([dot(table, halved(chosen)) for table in tables])
    row_half = counted((QROWS, HALF), 0) >= QROWS // 2
    lane = counted((QROWS, HALF), 1)
    same_side = row_half == (by_24(lane)[1] >= WLO)
    allowed = [
        same_side & ((lane >= 72) | (lat > 0)),
        same_side & ((lane < 72) | (lat < lat_last)),
    ]

    def bias_of(lat_window, entry):
        at = entry * GROUP
        terms = jnp.concatenate([s[lat_window][at : at + GROUP] for s in spreads], axis=0)
        return jnp.where(allowed[lat_window], terms, FAR)

    w_q = qkv_ref[:, :D]
    w_k = qkv_ref[:, D : 2 * D]
    w_v = qkv_ref[:, 2 * D :]

    def asked_of(n):
        queries = halved(dot(n, w_q))
        keys = halved(dot(n, w_k))
        values = halved(dot(n, w_v))
        out = []
        for lat_window in range(2):
            rows = slice(lat_window * HALF, (lat_window + 1) * HALF)
            asked = halved(dot(picks[lat_window], queries[rows])) * owned
            out.append((asked, dot_t(asked, keys[rows]) * HEAD_DIM**-0.5, values[rows]))
        return out

    for lat_window, (asked, scores, values) in enumerate(asked_of(pair_cells_ref[...])):
        asked_ref[lat_window] = asked
        value_ref[lat_window] = values
        score_ref[lat_window] = scores + bias_of(lat_window, 1)
        bias_ref[lat_window] = bias_of(lat_window, 2)

    parts = []
    for lat_window, (asked, scores, values) in enumerate(asked_of(halved(normalized(alone_cells_ref[...].astype(jnp.float32), gain1_ref[...])))):
        parts.append(softmax_context([scores + bias_of(lat_window, 0)], [values], owned))
    alone = finish(
        alone_own,
        parts,
        back,
        proj_ref[...],
        gain2_ref[...],
        fc1_ref[...],
        fc2_ref[...],
    )
    alone_ref[...] = dot(halved(jnp.where(woven_row == lev, 1.0, 0.0)), alone)


def late_kernel(
    other_ref,
    alone_ref,
    own_ref,
    asked_ref,
    value_ref,
    score_ref,
    bias_ref,
    owned_ref,
    back_ref,
    woven_ref,
    qkv_ref,
    proj_ref,
    fc1_ref,
    fc2_ref,
    gain2_ref,
    out_ref,
):
    owned = owned_ref[...]
    packed = other_ref[...]
    keys = packed_dots(packed, qkv_ref[:, D : 2 * D])
    values = packed_dots(packed, qkv_ref[:, 2 * D :])
    parts = []
    for lat_window in range(2):
        scores = dot_t(asked_ref[lat_window], keys[lat_window]) * HEAD_DIM**-0.5 + bias_ref[lat_window]
        parts.append(
            softmax_context(
                [score_ref[lat_window], scores], [value_ref[lat_window], values[lat_window]], owned
            )
        )
    pair = finish(
        own_ref[...],
        parts,
        (back_ref[0], back_ref[1]),
        proj_ref[...],
        gain2_ref[...],
        fc1_ref[...],
        fc2_ref[...],
    )
    result = halved(alone_ref[...] + dot(woven_ref[...], pair))
    out_ref[...] = result.reshape(72, 2, D)


def pairs_of(size, crossed):
    shift = 1 if crossed else 0
    return [[(2 * i + shift) % size, (2 * i + 1 + shift) % size] for i in range(size // 2)]


def swapped(block, axis, crossed):
    route = []
    for a, b in pairs_of(lax.axis_size(axis), crossed):
        route += [(a, b), (b, a)]
    return lax.ppermute(block, axis, route)


def per_device(
    tokens, norm1_gain, qkv_weight, proj_weight, earth_bias, norm2_gain, fc1_weight, fc2_weight
):
    lon_size = lax.axis_size("lon")
    lat_size = lax.axis_size("lat")

    cells_t = tokens.transpose(1, 2, 0, 3)
    tables_t = earth_bias[:, 0].transpose(1, 0, 2)
    params = pltpu.CompilerParams(vmem_limit_bytes=VMEM_LIMIT)
    half_t = pl.pallas_call(
        half_kernel,
        out_shape=pltpu.VMEM((WLA, HLO, 2, D), jnp.bfloat16),
        in_specs=[pl.BlockSpec(memory_space=pltpu.HBM)],
        out_specs=pl.BlockSpec(memory_space=pltpu.VMEM),
        scratch_shapes=[pltpu.SemaphoreType.DMA],
        compiler_params=pltpu.CompilerParams(vmem_limit_bytes=VMEM_LIMIT),
        name="half",
    )(pltpu.with_memory_space_constraint(cells_t, pltpu.HBM))
    far = swapped(half_t, "lon", True)
    joint = lax.all_gather(
        cells_t, "lon", axis_index_groups=pairs_of(lon_size, False), axis=1, tiled=True
    )
    whole = pl.BlockSpec(memory_space=pltpu.VMEM)
    placed = pltpu.with_memory_space_constraint
    held = lambda x: placed(x, pltpu.VMEM)
    sent = pltpu.VMEM((SENT + TABLE, LANES), jnp.bfloat16)
    wide, lower, sent_far, sent_near = pl.pallas_call(
        pack_kernel,
        out_shape=[
            pltpu.VMEM((ROWS, D), jnp.bfloat16),
            pltpu.VMEM((TABLE, WLA * SPAN), jnp.bfloat16),
            sent,
            sent,
        ],
        in_specs=[whole] * 3,
        out_specs=[whole] * 4,
        compiler_params=params,
        name="pack",
    )(
        held(far),
        held(joint),
        held(tables_t),
    )
    lat_far = swapped(sent_far, "lat", True)
    lat_both = lax.all_gather(sent_near, "lat", axis_index_groups=pairs_of(lat_size, False))
    gain1 = held(norm1_gain.reshape(1, D))
    level = pltpu.VMEM((ROWS, D), jnp.bfloat16)
    gain2, alone_cells, pair_cells, upper, sent = pl.pallas_call(
        assemble_kernel,
        out_shape=[
            pltpu.VMEM((1, D), jnp.float32),
            level,
            level,
            pltpu.VMEM((TABLE, WLA * SPAN), jnp.bfloat16),
            pltpu.VMEM((HALF + 72, LANES), jnp.bfloat16),
        ],
        in_specs=[whole] * 5,
        out_specs=[whole] * 5,
        compiler_params=params,
        name="assemble",
    )(held(lat_far), held(lat_both), wide, gain1, held(norm2_gain.reshape(1, D)))
    other = swapped(sent, "lev", False)

    shared = (
        qkv_weight,
        proj_weight,
        fc1_weight,
        fc2_weight.T,
        gain2,
    )
    passed = [
        pltpu.VMEM((CELLS, D), jnp.float32),
        pltpu.VMEM((72, D), jnp.float32),
        pltpu.VMEM((2, QROWS, D), jnp.bfloat16),
        pltpu.VMEM((2, HALF, D), jnp.bfloat16),
        pltpu.VMEM((2, QROWS, HALF), jnp.float32),
        pltpu.VMEM((2, QROWS, HALF), jnp.float32),
        pltpu.VMEM((QROWS, D), jnp.bfloat16),
        pltpu.VMEM((2, 72, QROWS), jnp.bfloat16),
        pltpu.VMEM((CELLS, 72), jnp.bfloat16),
    ]
    shared = [held(x) for x in shared]
    early = pl.pallas_call(
        early_kernel,
        out_shape=passed,
        in_specs=[whole] * (6 + len(shared)),
        out_specs=[whole] * len(passed),
        cost_estimate=pl.CostEstimate(flops=4_000_000_000, transcendentals=0, bytes_accessed=0),
        compiler_params=params,
        name="early",
    )(alone_cells, pair_cells, wide, gain1, upper, lower, *shared)
    result = pl.pallas_call(
        late_kernel,
        out_shape=jax.ShapeDtypeStruct((72, 2, D), jnp.bfloat16),
        in_specs=[whole] * 15,
        out_specs=whole,
        compiler_params=params,
        name="late",
    )(held(other), *early, *shared)
    return result.reshape(WLA, WLO, 2, D).transpose(2, 0, 1, 3)


def solution(mesh):
    placed = (
        P("lev", "lat", "lon", None),
        P(),
        P(),
        P(),
        P(None, "lat", None, None),
        P(),
        P(),
        P(),
    )
    return jax.shard_map(
        per_device,
        mesh=mesh,
        in_specs=placed,
        out_specs=P("lev", "lat", "lon", None),
        check_vma=False,
    )
```

```python
import jax
import jax.numpy as jnp
from jax import lax
from jax.experimental import pallas as pl
from jax.experimental.pallas import tpu as pltpu
from jax.sharding import PartitionSpec as P

D = 192
HEADS = 6
HEAD_DIM = 32
WLA = 6
WLO = 12
HLA = 3
HLO = 6
SPAN = 2 * WLO - 1
ROWS = 288
HALF = 144
QROWS = 216
GROUP = 18
FAR = -1e30
LANES = 256
TABLE = 54
CELLS = 144
SENT = 112
FAR_COLUMNS = 12
VMEM_LIMIT = 16 * 1024 * 1024

norm_eps = 1e-05


def counted(shape, dim):
    return lax.broadcasted_iota(jnp.int32, shape, dim)


def by_24(n):
    quotient = (n * 2731) >> 16
    return quotient, n - 24 * quotient


def by_18(n):
    quotient = (n * 3641) >> 16
    return quotient, n - 18 * quotient


def by_3(n):
    quotient = (n * 21846) >> 16
    return quotient, n - 3 * quotient


def one_hot(target, width):
    shape = (target.shape[0], width)
    return halved(jnp.where(counted(shape, 1) == target, 1.0, 0.0))


def normalized(values, gain):
    average = jnp.mean(values, axis=-1, keepdims=True)
    centered = values - average
    variance = jnp.mean(centered * centered, axis=-1, keepdims=True)
    return centered * lax.rsqrt(variance + norm_eps) * gain


def dot(a, b):
    return jnp.dot(a, b, preferred_element_type=jnp.float32)


def dot_t(a, b):
    return lax.dot_general(a, b, (((1,), (1,)), ((), ())), preferred_element_type=jnp.float32)


def halved(x):
    return x.astype(jnp.bfloat16)


def softmax_context(scores, values, owned):
    top = jnp.max(scores[0], axis=-1, keepdims=True)
    for s in scores[1:]:
        top = jnp.maximum(top, jnp.max(s, axis=-1, keepdims=True))
    weights = [jnp.exp(s - top) for s in scores]
    total = jnp.sum(weights[0], axis=-1, keepdims=True)
    for w in weights[1:]:
        total = total + jnp.sum(w, axis=-1, keepdims=True)
    inverse = 1.0 / total
    context = 0.0
    for w, v in zip(weights, values):
        context = context + dot(halved(w * inverse), v)
    return halved(context) * owned


def finish(own, parts, back, proj, gain, fc1, fc2_t):
    context = halved(dot(back[0], parts[0]) + dot(back[1], parts[1]))
    first = own + dot(context, proj)
    mixed = dot(halved(normalized(first, gain)), fc1)
    hidden = halved(mixed * (1.0 + lax.erf(mixed * (0.5**0.5))) * 0.5)
    return halved(first + dot_t(hidden, fc2_t))


def pack_kernel(
    far_ref, joint_ref, tables_ref,
    wide_ref, lower_ref, sent_far_ref, sent_near_ref,
):
    lev = lax.axis_index("lev")
    lat_even = lax.axis_index("lat") % 2 == 0
    odd = lax.axis_index("lon") % 2
    joint = joint_ref[...].reshape(ROWS, D)
    far = far_ref[...].reshape(2 * WLA * FAR_COLUMNS, D)
    row = counted((ROWS, 1), 0)
    level = (row >= HALF).astype(jnp.int32)
    cell = row - HALF * level
    lat_row, column = by_24(cell)
    from_far = odd * (column - WLO - HLO) + (1 - odd) * (HLO - 1 - column) >= 0
    near_cell = cell + HLO * (2 * odd - 1)
    far_cell = lat_row * FAR_COLUMNS + column
    far_cell = far_cell + (1 - odd) * (FAR_COLUMNS - HLO) - odd * (WLO + HLO)
    near_pick = one_hot(jnp.where(from_far, -1, 2 * near_cell + level), ROWS)
    far_pick = one_hot(jnp.where(from_far, 2 * far_cell + level, -1), 2 * WLA * FAR_COLUMNS)
    wide = dot(near_pick, joint) + dot(far_pick, far)
    wide_ref[...] = halved(wide)
    head = jnp.concatenate([wide[:72], wide[HALF : HALF + 72]], axis=0)
    tail = jnp.concatenate([wide[72:HALF], wide[HALF + 72 :]], axis=0)

    tables = tables_ref[...].reshape(2 * HEADS, 4 * WLA * WLA * SPAN)
    kinds = [dot(one_hot(2 * counted((8, 1), 0) + i, 2 * HEADS), tables) for i in range(2)]
    width = WLA * WLA * SPAN
    part = lambda i, at: kinds[i][:HEADS, at * width : (at + 1) * width]
    entries = [
        jnp.where(lev == 0, part(1, 3), part(1, 0)),
        jnp.where(lev == 0, part(0, 0), part(0, 3)),
        jnp.where(lev == 0, part(0, 1), part(0, 2)),
    ]
    span = WLA * SPAN
    rows = [
        jnp.concatenate(
            [e[:, (at + a) * span : (at + a + 1) * span] for e in entries for a in range(HLA)],
            axis=0,
        )
        for at in (0, HLA)
    ]
    lower_ref[...] = halved(rows[0])
    upper = jnp.concatenate([rows[1], jnp.zeros((TABLE, LANES - span), jnp.float32)], axis=1)
    for ref, cells in (
        (sent_far_ref, jnp.where(lat_even, head, tail)),
        (sent_near_ref, jnp.where(lat_even, tail, head)),
    ):
        second = cells[72:]
        rest = second[:, LANES - D :]
        ref[:72] = halved(jnp.concatenate([cells[:72], second[:, : LANES - D]], axis=1))
        ref[72:SENT] = halved(jnp.concatenate([rest[:40], rest[32:]], axis=1))
        ref[SENT:] = halved(upper)


def assemble_kernel(
    near_ref, both_ref, wide_ref, gain_ref, gain2_ref, gain2_out, alone_ref, pair_ref, table_ref, sent_ref
):
    lev = lax.axis_index("lev")
    lat_odd = lax.axis_index("lat") % 2
    near = near_ref[...].astype(jnp.float32)
    far = both_ref[lat_odd].astype(jnp.float32)
    wide = wide_ref[...].astype(jnp.float32)
    before = jnp.where(lat_odd == 0, far, near)
    after = jnp.where(lat_odd == 0, near, far)

    def unpacked(rows):
        rest = [rows[72:SENT, : LANES // 2], rows[80:SENT, LANES // 2 :]]
        second = [rows[:72, D:], jnp.concatenate(rest, axis=0)]
        return rows[:72, :D], jnp.concatenate(second, axis=1)

    edges = unpacked(before), unpacked(after)
    levels = [
        jnp.concatenate(
            [
                edges[0][l],
                wide[l * HALF : (l + 1) * HALF],
                edges[1][l],
            ],
            axis=0,
        )
        for l in range(2)
    ]
    gain2_out[...] = gain2_ref[...]
    pair = normalized(jnp.where(lev == 0, levels[1], levels[0]), gain_ref[...])
    pair_ref[...] = halved(pair)
    first = pair[:HALF]
    second = pair[HALF:]
    sent_ref[:HALF] = halved(jnp.concatenate([first, second[:, : LANES - D]], axis=1))
    rest = second[:, LANES - D :]
    sent_ref[HALF:] = halved(jnp.concatenate([rest[:72], rest[72:]], axis=1))
    alone_ref[...] = halved(jnp.where(lev == 0, levels[0], levels[1]))
    table_ref[...] = halved(before[SENT:, : WLA * SPAN])


def packed_dots(packed, weight):
    spare = jnp.zeros((LANES - D, weight.shape[1]), weight.dtype)
    first = dot(packed[:HALF], jnp.concatenate([weight, spare], axis=0))
    low = jnp.concatenate([spare, weight[: LANES - D]], axis=0)
    second = dot(packed[:HALF, LANES // 2 :], low)
    high = weight[LANES - D :]
    rest = [dot(packed[HALF:, : LANES // 2], high), dot(packed[HALF:, LANES // 2 :], high)]
    return halved(first), halved(second + jnp.concatenate(rest, axis=0))


def early_kernel(
    alone_cells_ref,
    pair_cells_ref,
    wide_ref,
    gain1_ref,
    upper_ref,
    lower_ref,
    qkv_ref,
    proj_ref,
    fc1_ref,
    fc2_ref,
    gain2_ref,
    alone_ref,
    own_ref,
    asked_ref,
    value_ref,
    score_ref,
    bias_ref,
    owned_ref,
    back_ref,
    woven_ref,
):
    lev = lax.axis_index("lev")
    lat = lax.axis_index("lat")
    lat_last = lax.axis_size("lat") - 1
    column, spot = by_18(counted((QROWS, 1), 0))
    head, place = by_3(spot)
    picks = [one_hot((at + place) * 24 + HLO + column, HALF) for at in (HLA, 0)]
    owned = halved(jnp.where(counted((QROWS, D), 1) >> 5 == head, 1.0, 0.0))
    owned_ref[...] = owned
    column, spot = by_18(counted((1, QROWS), 1))
    source = by_3(spot)[1] * WLO + column
    cell = counted((72, QROWS), 0)
    back = [halved(jnp.where(cell == source + at * WLO, 1.0, 0.0)) for at in (0, HLA)]
    for at in range(2):
        back_ref[at] = back[at]
    wide = wide_ref[...]
    place = counted((72, 1), 0)
    lat_row = (place * 5462) >> 16
    cell = lat_row * 24 + HLO + place - WLO * lat_row
    own_ref[...] = dot(one_hot(cell + HALF * (1 - lev), ROWS), wide)
    alone_own = dot(one_hot(cell + HALF * lev, ROWS), wide)
    woven_row = counted((CELLS, 72), 0) - 2 * counted((CELLS, 72), 1)
    woven_ref[...] = halved(jnp.where(woven_row == 1 - lev, 1.0, 0.0))
    entry, spot = by_18(counted((3 * GROUP, 1), 0))
    head, place = by_3(spot)
    gaps = one_hot((entry * HLA + place) * HEADS + head, TABLE)
    span = WLA * SPAN
    tables = [halved(dot(gaps, ref[...])) for ref in (upper_ref, lower_ref)]
    lat_place, column = by_24(counted((span, HALF), 1))
    offset = counted((span, HALF), 0) - (lat_place * SPAN + 17 - column)
    sides = [jnp.where(column < WLO, offset, -1), jnp.where(column < WLO, -1, offset)]
    spreads = []
    for o in range(WLO):
        chosen = jnp.where(sides[o >= HLO] == o, 1.0, 0.0)
        spreads.append([dot(table, halved(chosen)) for table in tables])
    row_half = counted((QROWS, HALF), 0) >= QROWS // 2
    lane = counted((QROWS, HALF), 1)
    same_side = row_half == (by_24(lane)[1] >= WLO)
    allowed = [
        same_side & ((lane >= 72) | (lat > 0)),
        same_side & ((lane < 72) | (lat < lat_last)),
    ]

    def bias_of(lat_window, entry):
        at = entry * GROUP
        terms = jnp.concatenate([s[lat_window][at : at + GROUP] for s in spreads], axis=0)
        return jnp.where(allowed[lat_window], terms, FAR)

    w_q = qkv_ref[:, :D]
    w_k = qkv_ref[:, D : 2 * D]
    w_v = qkv_ref[:, 2 * D :]

    def asked_of(n):
        queries = halved(dot(n, w_q))
        keys = halved(dot(n, w_k))
        values = halved(dot(n, w_v))
        out = []
        for lat_window in range(2):
            rows = slice(lat_window * HALF, (lat_window + 1) * HALF)
            asked = halved(dot(picks[lat_window], queries[rows])) * owned
            out.append((asked, dot_t(asked, keys[rows]) * HEAD_DIM**-0.5, values[rows]))
        return out

    for lat_window, (asked, scores, values) in enumerate(asked_of(pair_cells_ref[...])):
        asked_ref[lat_window] = asked
        value_ref[lat_window] = values
        score_ref[lat_window] = scores + bias_of(lat_window, 1)
        bias_ref[lat_window] = bias_of(lat_window, 2)

    parts = []
    for lat_window, (asked, scores, values) in enumerate(asked_of(halved(normalized(alone_cells_ref[...].astype(jnp.float32), gain1_ref[...])))):
        parts.append(softmax_context([scores + bias_of(lat_window, 0)], [values], owned))
    alone = finish(
        alone_own,
        parts,
        back,
        proj_ref[...],
        gain2_ref[...],
        fc1_ref[...],
        fc2_ref[...],
    )
    alone_ref[...] = dot(halved(jnp.where(woven_row == lev, 1.0, 0.0)), alone)


def late_kernel(
    other_ref,
    alone_ref,
    own_ref,
    asked_ref,
    value_ref,
    score_ref,
    bias_ref,
    owned_ref,
    back_ref,
    woven_ref,
    qkv_ref,
    proj_ref,
    fc1_ref,
    fc2_ref,
    gain2_ref,
    out_ref,
):
    owned = owned_ref[...]
    packed = other_ref[...]
    keys = packed_dots(packed, qkv_ref[:, D : 2 * D])
    values = packed_dots(packed, qkv_ref[:, 2 * D :])
    parts = []
    for lat_window in range(2):
        scores = dot_t(asked_ref[lat_window], keys[lat_window]) * HEAD_DIM**-0.5 + bias_ref[lat_window]
        parts.append(
            softmax_context(
                [score_ref[lat_window], scores], [value_ref[lat_window], values[lat_window]], owned
            )
        )
    pair = finish(
        own_ref[...],
        parts,
        (back_ref[0], back_ref[1]),
        proj_ref[...],
        gain2_ref[...],
        fc1_ref[...],
        fc2_ref[...],
    )
    result = halved(alone_ref[...] + dot(woven_ref[...], pair))
    out_ref[...] = result.reshape(72, 2, D)


def pairs_of(size, crossed):
    shift = 1 if crossed else 0
    return [[(2 * i + shift) % size, (2 * i + 1 + shift) % size] for i in range(size // 2)]


def swapped(block, axis, crossed):
    route = []
    for a, b in pairs_of(lax.axis_size(axis), crossed):
        route += [(a, b), (b, a)]
    return lax.ppermute(block, axis, route)


def per_device(
    tokens, norm1_gain, qkv_weight, proj_weight, earth_bias, norm2_gain, fc1_weight, fc2_weight
):
    lon_size = lax.axis_size("lon")
    lat_size = lax.axis_size("lat")

    cells_t = tokens.transpose(1, 2, 0, 3)
    tables_t = earth_bias[:, 0].transpose(1, 0, 2)
    params = pltpu.CompilerParams(vmem_limit_bytes=VMEM_LIMIT)
    far = swapped(cells_t, "lon", True)
    joint = lax.all_gather(
        cells_t, "lon", axis_index_groups=pairs_of(lon_size, False), axis=1, tiled=True
    )
    whole = pl.BlockSpec(memory_space=pltpu.VMEM)
    placed = pltpu.with_memory_space_constraint
    held = lambda x: placed(x, pltpu.VMEM)
    sent = pltpu.VMEM((SENT + TABLE, LANES), jnp.bfloat16)
    wide, lower, sent_far, sent_near = pl.pallas_call(
        pack_kernel,
        out_shape=[
            pltpu.VMEM((ROWS, D), jnp.bfloat16),
            pltpu.VMEM((TABLE, WLA * SPAN), jnp.bfloat16),
            sent,
            sent,
        ],
        in_specs=[whole] * 3,
        out_specs=[whole] * 4,
        compiler_params=params,
        name="pack",
    )(
        held(far),
        held(joint),
        held(tables_t),
    )
    lat_near = swapped(sent_near, "lat", False)
    lat_both = lax.all_gather(sent_far, "lat", axis_index_groups=pairs_of(lat_size, True))
    gain1 = held(norm1_gain.reshape(1, D))
    level = pltpu.VMEM((ROWS, D), jnp.bfloat16)
    gain2, alone_cells, pair_cells, upper, sent = pl.pallas_call(
        assemble_kernel,
        out_shape=[
            pltpu.VMEM((1, D), jnp.float32),
            level,
            level,
            pltpu.VMEM((TABLE, WLA * SPAN), jnp.bfloat16),
            pltpu.VMEM((HALF + 72, LANES), jnp.bfloat16),
        ],
        in_specs=[whole] * 5,
        out_specs=[whole] * 5,
        compiler_params=params,
        name="assemble",
    )(held(lat_near), held(lat_both), wide, gain1, held(norm2_gain.reshape(1, D)))
    other = swapped(sent, "lev", False)

    shared = (
        qkv_weight,
        proj_weight,
        fc1_weight,
        fc2_weight.T,
        gain2,
    )
    passed = [
        pltpu.VMEM((CELLS, D), jnp.float32),
        pltpu.VMEM((72, D), jnp.float32),
        pltpu.VMEM((2, QROWS, D), jnp.bfloat16),
        pltpu.VMEM((2, HALF, D), jnp.bfloat16),
        pltpu.VMEM((2, QROWS, HALF), jnp.float32),
        pltpu.VMEM((2, QROWS, HALF), jnp.float32),
        pltpu.VMEM((QROWS, D), jnp.bfloat16),
        pltpu.VMEM((2, 72, QROWS), jnp.bfloat16),
        pltpu.VMEM((CELLS, 72), jnp.bfloat16),
    ]
    shared = [held(x) for x in shared]
    early = pl.pallas_call(
        early_kernel,
        out_shape=passed,
        in_specs=[whole] * (6 + len(shared)),
        out_specs=[whole] * len(passed),
        cost_estimate=pl.CostEstimate(flops=4_000_000_000, transcendentals=0, bytes_accessed=0),
        compiler_params=params,
        name="early",
    )(alone_cells, pair_cells, wide, gain1, upper, lower, *shared)
    result = pl.pallas_call(
        late_kernel,
        out_shape=jax.ShapeDtypeStruct((72, 2, D), jnp.bfloat16),
        in_specs=[whole] * 15,
        out_specs=whole,
        compiler_params=params,
        name="late",
    )(held(other), *early, *shared)
    return result.reshape(WLA, WLO, 2, D).transpose(2, 0, 1, 3)


def solution(mesh):
    placed = (
        P("lev", "lat", "lon", None),
        P(),
        P(),
        P(),
        P(None, "lat", None, None),
        P(),
        P(),
        P(),
    )
    return jax.shard_map(
        per_device,
        mesh=mesh,
        in_specs=placed,
        out_specs=P("lev", "lat", "lon", None),
        check_vma=False,
    )
```

```python
import jax
import jax.numpy as jnp
from jax import lax
from jax.experimental import pallas as pl
from jax.experimental.pallas import tpu as pltpu
from jax.sharding import PartitionSpec as P

D = 192
HEADS = 6
HEAD_DIM = 32
WLA = 6
WLO = 12
HLA = 3
HLO = 6
SPAN = 2 * WLO - 1
ROWS = 288
HALF = 144
QROWS = 216
GROUP = 18
FAR = -1e30
LANES = 256
TABLE = 54
CELLS = 144
SENT = 112
FAR_COLUMNS = 6
VMEM_LIMIT = 16 * 1024 * 1024

norm_eps = 1e-05


def counted(shape, dim):
    return lax.broadcasted_iota(jnp.int32, shape, dim)


def by_24(n):
    quotient = (n * 2731) >> 16
    return quotient, n - 24 * quotient


def by_18(n):
    quotient = (n * 3641) >> 16
    return quotient, n - 18 * quotient


def by_3(n):
    quotient = (n * 21846) >> 16
    return quotient, n - 3 * quotient


def one_hot(target, width):
    shape = (target.shape[0], width)
    return halved(jnp.where(counted(shape, 1) == target, 1.0, 0.0))


def normalized(values, gain):
    average = jnp.mean(values, axis=-1, keepdims=True)
    centered = values - average
    variance = jnp.mean(centered * centered, axis=-1, keepdims=True)
    return centered * lax.rsqrt(variance + norm_eps) * gain


def dot(a, b):
    return jnp.dot(a, b, preferred_element_type=jnp.float32)


def dot_t(a, b):
    return lax.dot_general(a, b, (((1,), (1,)), ((), ())), preferred_element_type=jnp.float32)


def halved(x):
    return x.astype(jnp.bfloat16)


def softmax_context(scores, values, owned):
    top = jnp.max(scores[0], axis=-1, keepdims=True)
    for s in scores[1:]:
        top = jnp.maximum(top, jnp.max(s, axis=-1, keepdims=True))
    weights = [jnp.exp(s - top) for s in scores]
    total = jnp.sum(weights[0], axis=-1, keepdims=True)
    for w in weights[1:]:
        total = total + jnp.sum(w, axis=-1, keepdims=True)
    inverse = 1.0 / total
    context = 0.0
    for w, v in zip(weights, values):
        context = context + dot(halved(w * inverse), v)
    return halved(context) * owned


def finish(own, parts, back, proj, gain, fc1, fc2_t):
    context = halved(dot(back[0], parts[0]) + dot(back[1], parts[1]))
    first = own + dot(context, proj)
    mixed = dot(halved(normalized(first, gain)), fc1)
    hidden = halved(mixed * (1.0 + lax.erf(mixed * (0.5**0.5))) * 0.5)
    return halved(first + dot_t(hidden, fc2_t))


def half_kernel(cells_ref, half_ref, sem):
    odd = lax.axis_index("lon") % 2
    copy = pltpu.make_async_copy(cells_ref.at[:, pl.ds(HLO * odd, HLO)], half_ref, sem)
    copy.start()
    copy.wait()


def pack_kernel(
    far_ref, joint_ref, tables_ref,
    wide_ref, lower_ref, sent_far_ref, sent_near_ref,
):
    lev = lax.axis_index("lev")
    lat_even = lax.axis_index("lat") % 2 == 0
    odd = lax.axis_index("lon") % 2
    joint = joint_ref[...].reshape(ROWS, D)
    far = far_ref[...].reshape(2 * WLA * FAR_COLUMNS, D)
    row = counted((ROWS, 1), 0)
    level = (row >= HALF).astype(jnp.int32)
    cell = row - HALF * level
    lat_row, column = by_24(cell)
    from_far = odd * (column - WLO - HLO) + (1 - odd) * (HLO - 1 - column) >= 0
    near_cell = cell + HLO * (2 * odd - 1)
    far_cell = lat_row * FAR_COLUMNS + column
    far_cell = far_cell + (1 - odd) * (FAR_COLUMNS - HLO) - odd * (WLO + HLO)
    near_pick = one_hot(jnp.where(from_far, -1, 2 * near_cell + level), ROWS)
    far_pick = one_hot(jnp.where(from_far, 2 * far_cell + level, -1), 2 * WLA * FAR_COLUMNS)
    wide = dot(near_pick, joint) + dot(far_pick, far)
    wide_ref[...] = halved(wide)
    head = jnp.concatenate([wide[:72], wide[HALF : HALF + 72]], axis=0)
    tail = jnp.concatenate([wide[72:HALF], wide[HALF + 72 :]], axis=0)

    tables = tables_ref[...].reshape(2 * HEADS, 4 * WLA * WLA * SPAN)
    kinds = [dot(one_hot(2 * counted((8, 1), 0) + i, 2 * HEADS), tables) for i in range(2)]
    width = WLA * WLA * SPAN
    part = lambda i, at: kinds[i][:HEADS, at * width : (at + 1) * width]
    entries = [
        jnp.where(lev == 0, part(1, 3), part(1, 0)),
        jnp.where(lev == 0, part(0, 0), part(0, 3)),
        jnp.where(lev == 0, part(0, 1), part(0, 2)),
    ]
    span = WLA * SPAN
    rows = [
        jnp.concatenate(
            [e[:, (at + a) * span : (at + a + 1) * span] for e in entries for a in range(HLA)],
            axis=0,
        )
        for at in (0, HLA)
    ]
    lower_ref[...] = halved(rows[0])
    upper = jnp.concatenate([rows[1], jnp.zeros((TABLE, LANES - span), jnp.float32)], axis=1)
    for ref, cells in (
        (sent_far_ref, jnp.where(lat_even, head, tail)),
        (sent_near_ref, jnp.where(lat_even, tail, head)),
    ):
        second = cells[72:]
        rest = second[:, LANES - D :]
        ref[:72] = halved(jnp.concatenate([cells[:72], second[:, : LANES - D]], axis=1))
        ref[72:SENT] = halved(jnp.concatenate([rest[:40], rest[32:]], axis=1))
        ref[SENT:] = halved(upper)


def assemble_kernel(
    near_ref, both_ref, wide_ref, gain_ref, gain2_ref, gain2_out, alone_ref, pair_ref, table_ref, sent_ref
):
    lev = lax.axis_index("lev")
    lat_odd = lax.axis_index("lat") % 2
    near = near_ref[...].astype(jnp.float32)
    far = both_ref[lat_odd].astype(jnp.float32)
    wide = wide_ref[...].astype(jnp.float32)
    before = jnp.where(lat_odd == 0, far, near)
    after = jnp.where(lat_odd == 0, near, far)

    def unpacked(rows):
        rest = [rows[72:SENT, : LANES // 2], rows[80:SENT, LANES // 2 :]]
        second = [rows[:72, D:], jnp.concatenate(rest, axis=0)]
        return rows[:72, :D], jnp.concatenate(second, axis=1)

    edges = unpacked(before), unpacked(after)
    levels = [
        jnp.concatenate(
            [
                edges[0][l],
                wide[l * HALF : (l + 1) * HALF],
                edges[1][l],
            ],
            axis=0,
        )
        for l in range(2)
    ]
    gain2_out[...] = gain2_ref[...]
    pair = normalized(jnp.where(lev == 0, levels[1], levels[0]), gain_ref[...])
    pair_ref[...] = halved(pair)
    first = pair[:HALF]
    second = pair[HALF:]
    sent_ref[:HALF] = halved(jnp.concatenate([first, second[:, : LANES - D]], axis=1))
    rest = second[:, LANES - D :]
    sent_ref[HALF:] = halved(jnp.concatenate([rest[:72], rest[72:]], axis=1))
    alone_ref[...] = halved(jnp.where(lev == 0, levels[0], levels[1]))
    table_ref[...] = halved(before[SENT:, : WLA * SPAN])


def packed_dots(packed, weight):
    spare = jnp.zeros((LANES - D, weight.shape[1]), weight.dtype)
    first = dot(packed[:HALF], jnp.concatenate([weight, spare], axis=0))
    low = jnp.concatenate([spare, weight[: LANES - D]], axis=0)
    second = dot(packed[:HALF, LANES // 2 :], low)
    high = weight[LANES - D :]
    rest = [dot(packed[HALF:, : LANES // 2], high), dot(packed[HALF:, LANES // 2 :], high)]
    return halved(first), halved(second + jnp.concatenate(rest, axis=0))


def early_kernel(
    alone_cells_ref,
    pair_cells_ref,
    wide_ref,
    gain1_ref,
    upper_ref,
    lower_ref,
    qkv_ref,
    proj_ref,
    fc1_ref,
    fc2_ref,
    gain2_ref,
    alone_ref,
    own_ref,
    asked_ref,
    value_ref,
    score_ref,
    bias_ref,
    owned_ref,
    back_ref,
    woven_ref,
):
    lev = lax.axis_index("lev")
    lat = lax.axis_index("lat")
    lat_last = lax.axis_size("lat") - 1
    column, spot = by_18(counted((QROWS, 1), 0))
    head, place = by_3(spot)
    picks = [one_hot((at + place) * 24 + HLO + column, HALF) for at in (HLA, 0)]
    owned = halved(jnp.where(counted((QROWS, D), 1) >> 5 == head, 1.0, 0.0))
    owned_ref[...] = owned
    column, spot = by_18(counted((1, QROWS), 1))
    source = by_3(spot)[1] * WLO + column
    cell = counted((72, QROWS), 0)
    back = [halved(jnp.where(cell == source + at * WLO, 1.0, 0.0)) for at in (0, HLA)]
    for at in range(2):
        back_ref[at] = back[at]
    wide = wide_ref[...]
    place = counted((72, 1), 0)
    lat_row = (place * 5462) >> 16
    cell = lat_row * 24 + HLO + place - WLO * lat_row
    own_ref[...] = dot(one_hot(cell + HALF * (1 - lev), ROWS), wide)
    alone_own = dot(one_hot(cell + HALF * lev, ROWS), wide)
    woven_row = counted((CELLS, 72), 0) - 2 * counted((CELLS, 72), 1)
    woven_ref[...] = halved(jnp.where(woven_row == 1 - lev, 1.0, 0.0))
    entry, spot = by_18(counted((3 * GROUP, 1), 0))
    head, place = by_3(spot)
    gaps = one_hot((entry * HLA + place) * HEADS + head, TABLE)
    span = WLA * SPAN
    tables = [halved(dot(gaps, ref[...])) for ref in (upper_ref, lower_ref)]
    lat_place, column = by_24(counted((span, HALF), 1))
    offset = counted((span, HALF), 0) - (lat_place * SPAN + 17 - column)
    sides = [jnp.where(column < WLO, offset, -1), jnp.where(column < WLO, -1, offset)]
    spreads = []
    for o in range(WLO):
        chosen = jnp.where(sides[o >= HLO] == o, 1.0, 0.0)
        spreads.append([dot(table, halved(chosen)) for table in tables])
    row_half = counted((QROWS, HALF), 0) >= QROWS // 2
    lane = counted((QROWS, HALF), 1)
    same_side = row_half == (by_24(lane)[1] >= WLO)
    allowed = [
        same_side & ((lane >= 72) | (lat > 0)),
        same_side & ((lane < 72) | (lat < lat_last)),
    ]

    def bias_of(lat_window, entry):
        at = entry * GROUP
        terms = jnp.concatenate([s[lat_window][at : at + GROUP] for s in spreads], axis=0)
        return jnp.where(allowed[lat_window], terms, FAR)

    w_q = qkv_ref[:, :D]
    w_k = qkv_ref[:, D : 2 * D]
    w_v = qkv_ref[:, 2 * D :]

    def asked_of(n):
        queries = halved(dot(n, w_q))
        keys = halved(dot(n, w_k))
        values = halved(dot(n, w_v))
        out = []
        for lat_window in range(2):
            rows = slice(lat_window * HALF, (lat_window + 1) * HALF)
            asked = halved(dot(picks[lat_window], queries[rows])) * owned
            out.append((asked, dot_t(asked, keys[rows]) * HEAD_DIM**-0.5, values[rows]))
        return out

    for lat_window, (asked, scores, values) in enumerate(asked_of(pair_cells_ref[...])):
        asked_ref[lat_window] = asked
        value_ref[lat_window] = values
        score_ref[lat_window] = scores + bias_of(lat_window, 1)
        bias_ref[lat_window] = bias_of(lat_window, 2)

    parts = []
    for lat_window, (asked, scores, values) in enumerate(asked_of(halved(normalized(alone_cells_ref[...].astype(jnp.float32), gain1_ref[...])))):
        parts.append(softmax_context([scores + bias_of(lat_window, 0)], [values], owned))
    alone = finish(
        alone_own,
        parts,
        back,
        proj_ref[...],
        gain2_ref[...],
        fc1_ref[...],
        fc2_ref[...],
    )
    alone_ref[...] = dot(halved(jnp.where(woven_row == lev, 1.0, 0.0)), alone)


def late_kernel(
    other_ref,
    alone_ref,
    own_ref,
    asked_ref,
    value_ref,
    score_ref,
    bias_ref,
    owned_ref,
    back_ref,
    woven_ref,
    qkv_ref,
    proj_ref,
    fc1_ref,
    fc2_ref,
    gain2_ref,
    out_ref,
):
    owned = owned_ref[...]
    packed = other_ref[...]
    keys = packed_dots(packed, qkv_ref[:, D : 2 * D])
    values = packed_dots(packed, qkv_ref[:, 2 * D :])
    parts = []
    for lat_window in range(2):
        scores = dot_t(asked_ref[lat_window], keys[lat_window]) * HEAD_DIM**-0.5 + bias_ref[lat_window]
        parts.append(
            softmax_context(
                [score_ref[lat_window], scores], [value_ref[lat_window], values[lat_window]], owned
            )
        )
    pair = finish(
        own_ref[...],
        parts,
        (back_ref[0], back_ref[1]),
        proj_ref[...],
        gain2_ref[...],
        fc1_ref[...],
        fc2_ref[...],
    )
    result = halved(alone_ref[...] + dot(woven_ref[...], pair))
    out_ref[...] = result.reshape(72, 2, D)


def pairs_of(size, crossed):
    shift = 1 if crossed else 0
    return [[(2 * i + shift) % size, (2 * i + 1 + shift) % size] for i in range(size // 2)]


def swapped(block, axis, crossed):
    route = []
    for a, b in pairs_of(lax.axis_size(axis), crossed):
        route += [(a, b), (b, a)]
    return lax.ppermute(block, axis, route)


def per_device(
    tokens, norm1_gain, qkv_weight, proj_weight, earth_bias, norm2_gain, fc1_weight, fc2_weight
):
    lon_size = lax.axis_size("lon")
    lat_size = lax.axis_size("lat")

    cells_t = tokens.transpose(1, 2, 0, 3)
    tables_t = earth_bias[:, 0].transpose(1, 0, 2)
    params = pltpu.CompilerParams(vmem_limit_bytes=VMEM_LIMIT)
    half_t = pl.pallas_call(
        half_kernel,
        out_shape=pltpu.VMEM((WLA, HLO, 2, D), jnp.bfloat16),
        in_specs=[pl.BlockSpec(memory_space=pltpu.HBM)],
        out_specs=pl.BlockSpec(memory_space=pltpu.VMEM),
        scratch_shapes=[pltpu.SemaphoreType.DMA],
        compiler_params=pltpu.CompilerParams(vmem_limit_bytes=VMEM_LIMIT),
        name="half",
    )(pltpu.with_memory_space_constraint(cells_t, pltpu.HBM))
    far = swapped(half_t, "lon", True)
    joint = lax.all_gather(
        cells_t, "lon", axis_index_groups=pairs_of(lon_size, False), axis=1, tiled=True
    )
    whole = pl.BlockSpec(memory_space=pltpu.VMEM)
    placed = pltpu.with_memory_space_constraint
    held = lambda x: placed(x, pltpu.VMEM)
    sent = pltpu.VMEM((SENT + TABLE, LANES), jnp.bfloat16)
    wide, lower, sent_far, sent_near = pl.pallas_call(
        pack_kernel,
        out_shape=[
            pltpu.VMEM((ROWS, D), jnp.bfloat16),
            pltpu.VMEM((TABLE, WLA * SPAN), jnp.bfloat16),
            sent,
            sent,
        ],
        in_specs=[whole] * 3,
        out_specs=[whole] * 4,
        compiler_params=params,
        name="pack",
    )(
        held(far),
        held(joint),
        held(tables_t),
    )
    lat_near = swapped(sent_near, "lat", False)
    lat_both = lax.all_gather(sent_far, "lat", axis_index_groups=pairs_of(lat_size, True))
    gain1 = held(norm1_gain.reshape(1, D))
    level = pltpu.VMEM((ROWS, D), jnp.bfloat16)
    gain2, alone_cells, pair_cells, upper, sent = pl.pallas_call(
        assemble_kernel,
        out_shape=[
            pltpu.VMEM((1, D), jnp.float32),
            level,
            level,
            pltpu.VMEM((TABLE, WLA * SPAN), jnp.bfloat16),
            pltpu.VMEM((HALF + 72, LANES), jnp.bfloat16),
        ],
        in_specs=[whole] * 5,
        out_specs=[whole] * 5,
        compiler_params=params,
        name="assemble",
    )(held(lat_near), held(lat_both), wide, gain1, held(norm2_gain.reshape(1, D)))
    other = swapped(sent, "lev", False)

    shared = (
        qkv_weight,
        proj_weight,
        fc1_weight,
        fc2_weight.T,
        gain2,
    )
    passed = [
        pltpu.VMEM((CELLS, D), jnp.float32),
        pltpu.VMEM((72, D), jnp.float32),
        pltpu.VMEM((2, QROWS, D), jnp.bfloat16),
        pltpu.VMEM((2, HALF, D), jnp.bfloat16),
        pltpu.VMEM((2, QROWS, HALF), jnp.float32),
        pltpu.VMEM((2, QROWS, HALF), jnp.float32),
        pltpu.VMEM((QROWS, D), jnp.bfloat16),
        pltpu.VMEM((2, 72, QROWS), jnp.bfloat16),
        pltpu.VMEM((CELLS, 72), jnp.bfloat16),
    ]
    shared = [held(x) for x in shared]
    early = pl.pallas_call(
        early_kernel,
        out_shape=passed,
        in_specs=[whole] * (6 + len(shared)),
        out_specs=[whole] * len(passed),
        cost_estimate=pl.CostEstimate(flops=4_000_000_000, transcendentals=0, bytes_accessed=0),
        compiler_params=params,
        name="early",
    )(alone_cells, pair_cells, wide, gain1, upper, lower, *shared)
    result = pl.pallas_call(
        late_kernel,
        out_shape=jax.ShapeDtypeStruct((72, 2, D), jnp.bfloat16),
        in_specs=[whole] * 15,
        out_specs=whole,
        compiler_params=params,
        name="late",
    )(held(other), *early, *shared)
    return result.reshape(WLA, WLO, 2, D).transpose(2, 0, 1, 3)


def solution(mesh):
    placed = (
        P("lev", "lat", "lon", None),
        P(),
        P(),
        P(),
        P(None, "lat", None, None),
        P(),
        P(),
        P(),
    )
    return jax.shard_map(
        per_device,
        mesh=mesh,
        in_specs=placed,
        out_specs=P("lev", "lat", "lon", None),
        check_vma=False,
    )
```
